32 devices in a mesh: patch: 4 (over y, x), hid: 8 (over z, core).
Axes of the slice: x: 2, y: 2, z: 4, core: 2. Of those that a mesh axis runs over, the one named last changes fastest.
Arguments:
- frames: bfloat16 [4, 2, 16, 64, 512], P(None, None, 'patch', None, 'hid'), may hold values from -6 to 6
- hidden_start: bfloat16 [2, 16, 64, 512], P(None, 'patch', None, 'hid'), may hold values from -4 to 4
- cell_start: float32 [2, 16, 64, 512], P(None, 'patch', None, 'hid'), may hold values from -6 to 6
- input_weight: bfloat16 [3, 3, 512, 4, 512], P(None, None, None, None, 'hid'), may hold values from -0.09375 to 0.09375
- hidden_weight: bfloat16 [3, 3, 512, 4, 512], P(None, None, None, None, 'hid'), may hold values from -0.09375 to 0.09375
- gate_bias: float32 [4, 512], P(None, 'hid'), may hold values from -3 to 3
- first_weight: bfloat16 [3, 3, 512, 512], replicated, may hold values from -0.09375 to 0.09375
- first_bias: float32 [512], replicated, may hold values from -3 to 3
- second_weight: bfloat16 [3, 3, 512, 512], replicated, may hold values from -0.09375 to 0.09375
- second_bias: float32 [512], replicated, may hold values from -3 to 3
Outputs:
- decoded: bfloat16 [2, 16, 64, 512], P(None, 'patch', 'hid')
- cell_final: float32 [2, 16, 64, 512], P(None, 'patch', None, 'hid')
The draws below stay inside these ranges and needn't reach their ends.
All inputs are finite; a program needn't handle non-finite values.
Results may differ from the reference program's by a relative error of at most 0.0045.
Values may be sent and summed in bfloat16 or wider, within the bound.
No kernel may reach another device: no remote copies, remote signals or barrier semaphores. Data moves between devices by JAX's collectives and lax.ppermute only.
A program may use at most 128 MiB of HBM per device.

```python
import jax
import jax.numpy as jnp

C = 512
CIN = 512
W = 64
B = 2
STEPS = 4
H = 16


def shard_levels(stream_key, extent, pieces, low, top_value):
    loudness, own = 1.0, jax.random.fold_in(stream_key, 6)
    for dim, blocks in pieces:
        heights = jnp.exp(jax.random.uniform(jax.random.fold_in(own, dim), (blocks,), jnp.float32, low / len(pieces), top_value / len(pieces)))
        loudness = loudness * jnp.repeat(heights, extent[dim] // blocks).reshape([-1 if axis == dim else 1 for axis in range(len(extent))])
    return loudness


def normal_values(stream_key, shape, scale, limit, shards=(), dtype=jnp.bfloat16):
    level = shard_levels(stream_key, shape, shards, -0.22, 0.18) if shards else 1.0
    entries = jax.random.normal(stream_key, shape, jnp.float32) * scale * level
    return jnp.minimum(jnp.maximum(entries, -limit), limit).astype(dtype)


def setup_inputs(seed: int = 0) -> dict:
    keys = jax.random.split(jax.random.key(seed), 11)
    return {
        "frames": normal_values(keys[0], (STEPS, B, H, W, CIN), 1.0, 6.0, ((2, 4), (4, 8))),
        "hidden_start": normal_values(keys[1], (B, H, W, C), 0.5, 4.0, ((1, 4), (3, 8))),
        "cell_start": normal_values(keys[2], (B, H, W, C), 1.0, 6.0, ((1, 4), (3, 8)), jnp.float32),
        "input_weight": normal_values(keys[3], (3, 3, CIN, 4, C), (9 * CIN) ** -0.5, 0.09375, ((4, 8),)),
        "hidden_weight": normal_values(keys[4], (3, 3, C, 4, C), (9 * C) ** -0.5, 0.09375, ((4, 8),)),
        "gate_bias": normal_values(keys[5], (4, C), 0.5, 3.0, ((1, 8),), jnp.float32),
        "first_weight": normal_values(keys[6], (3, 3, C, C), (9 * C) ** -0.5, 0.09375),
        "first_bias": normal_values(keys[7], (C,), 0.5, 3.0, (), jnp.float32),
        "second_weight": normal_values(keys[8], (3, 3, C, C), (9 * C) ** -0.5, 0.09375),
        "second_bias": normal_values(keys[9], (C,), 0.5, 3.0, (), jnp.float32),
    }


FORGET_BIAS = 1.0


def conv_taps(padded, weight):
    batch_count, padded_rows, padded_cols, channel_count = padded.shape
    row_count = padded_rows - 2
    col_count = padded_cols - 2
    summed = jnp.zeros((batch_count * row_count * col_count, weight.shape[-1]), jnp.float32)
    for tap_row in range(3):
        for tap_col in range(3):
            window = padded[:, tap_row:tap_row + row_count, tap_col:tap_col + col_count, :]
            summed = summed + jnp.dot(window.reshape(-1, channel_count), weight[tap_row, tap_col], preferred_element_type=jnp.float32)
    return summed.reshape(batch_count, row_count, col_count, weight.shape[-1])


def lstm_update(gates, cell):
    shaped = gates.reshape(gates.shape[:-1] + (4, gates.shape[-1] // 4))
    input_gate = jax.nn.sigmoid(shaped[..., 0, :])
    forget_gate = jax.nn.sigmoid(shaped[..., 1, :] + FORGET_BIAS)
    candidate = jnp.tanh(shaped[..., 2, :])
    output_gate = jax.nn.sigmoid(shaped[..., 3, :])
    cell = forget_gate * cell + input_gate * candidate
    hidden = (output_gate * jnp.tanh(cell)).astype(jnp.bfloat16)
    return hidden, cell


def pad_both(image):
    return jnp.pad(image, ((0, 0), (1, 1), (1, 1), (0, 0)))


def reference(frames, hidden_start, cell_start, input_weight, hidden_weight, gate_bias, first_weight, first_bias, second_weight, second_bias):
    wide_input = input_weight.reshape(3, 3, CIN, 4 * C)
    wide_hidden = hidden_weight.reshape(3, 3, C, 4 * C)
    bias_row = gate_bias.reshape(-1)
    hidden = hidden_start
    cell = cell_start
    for time_index in range(STEPS):
        gates = conv_taps(pad_both(frames[time_index]), wide_input) + conv_taps(pad_both(hidden), wide_hidden) + bias_row
        hidden, cell = lstm_update(gates, cell)
    middle = jax.nn.silu(conv_taps(pad_both(hidden), first_weight) + first_bias).astype(jnp.bfloat16)
    decoded = (conv_taps(pad_both(middle), second_weight) + second_bias).astype(jnp.bfloat16)
    return decoded, cell
```

```python
import functools

import jax
import jax.numpy as jnp
from jax import lax
from jax.experimental import pallas as pl
from jax.experimental.pallas import tpu as pltpu
from jax.sharding import PartitionSpec as P

FORGET_BIAS = 1.0
VMEM_LIMIT = 14 * 1024 * 1024

NT = (((1,), (1,)), ((), ()))
NN = (((1,), (0,)), ((), ()))


def place_columns(dst, row0, pieces, group, cols, masked):
    count, width = pieces[0].shape
    groups = len(pieces)
    place = lax.rem(lax.broadcasted_iota(jnp.int32, (count, width), 0), cols)

    def shifts(piece):
        wide = piece.astype(jnp.float32)
        low = pltpu.roll(wide, 1, 0)
        high = pltpu.roll(wide, count - 1, 0)
        if masked:
            low = jnp.where(place == 0, 0.0, low)
            high = jnp.where(place == cols - 1, 0.0, high)
        return (low.astype(dst.dtype), wide.astype(dst.dtype), high.astype(dst.dtype))

    shifted = [shifts(piece) for piece in pieces]
    rows = pl.ds(row0, count)
    if width % 128 == 0:
        for k in range(groups):
            lanes = pl.ds(pl.multiple_of(lax.bitwise_xor(group, k) * width, width), width)
            for q in range(3):
                dst[q, rows, lanes] = shifted[k][q]
    else:
        for j in range(groups):

            @pl.when(group == j)
            def _():
                for q in range(3):
                    dst[q, rows, :] = jnp.concatenate(
                        [shifted[j ^ i][q] for i in range(groups)], axis=1
                    )


def halo_pieces(a_ref, b_ref):
    patch = lax.axis_index("patch")
    even = lax.rem(patch, 2) == 0
    above = patch > 0
    below = patch < lax.axis_size("patch") - 1
    top, bottom = [], []
    for k in range(a_ref.shape[1]):
        a = a_ref[0, k].astype(jnp.float32)
        b = b_ref[0, k].astype(jnp.float32)
        top.append(jnp.where(above, jnp.where(even, b, a), 0.0))
        bottom.append(jnp.where(below, jnp.where(even, a, b), 0.0))
    return top, bottom


def conv_kernel(groups, cols, halo, *refs):
    refs = list(refs)
    parts = [refs.pop(0) for _ in range(groups)]
    if halo:
        edge_a, edge_b = refs.pop(0), refs.pop(0)
    own_ref, pair_ref, init_ref, out_ref, held = refs
    count = out_ref.shape[1]
    step = pl.program_id(0)
    group = lax.axis_index("hid") // 2

    @pl.when(step == 0)
    def _():
        place_columns(held, cols, [part[0] for part in parts], group, cols, True)
        if halo:
            top, bottom = halo_pieces(edge_a, edge_b)
            place_columns(held, 0, top, group, cols, True)
            place_columns(held, cols + count, bottom, group, cols, True)
        else:
            zero = jnp.zeros((cols, held.shape[2]), held.dtype)
            for q in range(3):
                held[q, pl.ds(0, cols), :] = zero
                held[q, pl.ds(cols + count, cols), :] = zero
        out_ref[...] = jnp.broadcast_to(init_ref[...], out_ref.shape)

    total = out_ref[...]
    for q in range(3):
        window = held[q, pl.ds(pl.multiple_of(step * cols, cols), count), :]
        weight = jnp.concatenate([own_ref[0, q], pair_ref[0, q]], axis=0)
        total = total + lax.dot_general(weight, window, NT, preferred_element_type=jnp.float32)
    out_ref[...] = total


def gate_kernel(cols, edge_a, edge_b, own_ref, pair_ref, total_ref, cell_ref, hidden_ref, cell_out, held, turned, summed):
    step = pl.program_id(0)
    group = lax.axis_index("hid") // 2
    core = lax.rem(lax.axis_index("hid"), 2)
    count = total_ref.shape[1]
    channels = cell_ref.shape[1]
    side = 2 * cols

    @pl.when(step == 0)
    def _():
        top, bottom = halo_pieces(edge_a, edge_b)
        zero = jnp.zeros((cols, held.shape[2]), held.dtype)
        for q in range(3):
            held[q, pl.ds(cols, cols), :] = zero
            held[q, pl.ds(2 * cols, cols), :] = zero
        place_columns(held, 0, top, group, cols, True)
        place_columns(held, 3 * cols, bottom, group, cols, True)
        summed[...] = total_ref[...]

    def add(row0, lane0):
        total = summed[:, lane0 : lane0 + side]
        for q in range(3):
            window = held[q, row0 : row0 + side, :]
            weight = jnp.concatenate([own_ref[0, q], pair_ref[0, q]], axis=0)
            total = total + lax.dot_general(weight, window, NT, preferred_element_type=jnp.float32)
        summed[:, lane0 : lane0 + side] = total

    @pl.when(step == 0)
    def _():
        add(0, 0)

    @pl.when(step == 1)
    def _():
        add(side, count - side)
        for half in range(2):
            base = half * 4 * channels
            z0, z1, z2, z3 = (summed[base + i * channels : base + (i + 1) * channels, :] for i in range(4))
            cell = jax.nn.sigmoid(z1 + FORGET_BIAS) * cell_ref[half] + jax.nn.sigmoid(z0) * jnp.tanh(z2)
            cell_out[half] = cell
            rows = pl.ds(pl.multiple_of(lax.bitwise_xor(core, half) * channels, channels), channels)
            turned[rows, :] = jax.nn.sigmoid(z3) * jnp.tanh(cell)
        hidden_ref[...] = turned[...].T.astype(hidden_ref.dtype)


def decoder_kernel(groups, rows, width, margin, inner, *refs):
    parts = refs[:groups]
    edge_a, edge_b, first_ref, bias1_ref, second_ref, bias2_ref, out_ref, held, middle, total1, total2 = refs[groups:]
    step = pl.program_id(0)
    hid = lax.axis_index("hid")
    group = hid // 2
    patch = lax.axis_index("patch")
    image_rows = rows * lax.axis_size("patch")
    image_cols = inner * groups

    @pl.when(step == 0)
    def _():
        top, bottom = halo_pieces(edge_a, edge_b)
        place_columns(held, 0, top, group, width, False)
        place_columns(held, 2 * width, [part[...] for part in parts], group, width, False)
        place_columns(held, (2 + rows) * width, bottom, group, width, False)
        total1[...] = jnp.broadcast_to(bias1_ref[...], total1.shape)

    @pl.when(step < 3)
    def _():
        total = total1[...]
        for q in range(3):
            window = held[q, pl.ds(pl.multiple_of(step * width, width), (rows + 2) * width), :]
            total = total + lax.dot_general(window, first_ref[0, q], NN, preferred_element_type=jnp.float32)
        total1[...] = total

    @pl.when(step == 3)
    def _():
        value = total1[...]
        place = lax.broadcasted_iota(jnp.int32, value.shape, 0)
        row = patch * rows + place // width - 1
        col = group * inner - margin + lax.rem(place, width)
        inside = (row >= 0) & (row < image_rows) & (col >= 0) & (col < image_cols)
        value = jnp.where(inside, value * jax.nn.sigmoid(value), 0.0)
        value = value.astype(middle.dtype).astype(jnp.float32)
        count = value.shape[0]
        middle[0] = pltpu.roll(value, 1, 0).astype(middle.dtype)
        middle[1] = value.astype(middle.dtype)
        middle[2] = pltpu.roll(value, count - 1, 0).astype(middle.dtype)
        total2[...] = jnp.broadcast_to(bias2_ref[...], total2.shape)

    @pl.when(step >= 3)
    def _():
        total = total2[...]
        for q in range(3):
            window = middle[q, pl.ds(pl.multiple_of((step - 3) * width, width), rows * width), :]
            total = total + lax.dot_general(window, second_ref[0, q], NN, preferred_element_type=jnp.float32)
        total2[...] = total

        @pl.when(step == 5)
        def _():
            out_ref[...] = total.astype(out_ref.dtype)


def constant(shape, index=None):
    index = (0,) * len(shape) if index is None else index
    return pl.BlockSpec(shape, lambda i: index)


def params():
    return pltpu.CompilerParams(vmem_limit_bytes=VMEM_LIMIT, dimension_semantics=("arbitrary",))


def conv_call(parts, index, edges, own, pair, init, cols):
    groups = len(parts)
    _, count, width = parts[0].shape
    channels = own.shape[3]
    outs = 2 * own.shape[2]
    tap = pl.BlockSpec((1, 3) + own.shape[2:], lambda i: (i, 0, 0, 0))
    specs = [constant((1, count, width), (index, 0, 0))] * groups
    operands = list(parts)
    if edges is not None:
        specs += [constant((1,) + edges[0].shape[1:], (index, 0, 0, 0))] * 2
        operands += list(edges)
    specs += [tap, tap, constant(init.shape)]
    operands += [own, pair, init]
    return pl.pallas_call(
        functools.partial(conv_kernel, groups, cols, edges is not None),
        grid=(3,),
        in_specs=specs,
        out_specs=constant((outs, count)),
        out_shape=jax.ShapeDtypeStruct((outs, count), jnp.float32),
        scratch_shapes=[pltpu.VMEM((3, count + 2 * cols, channels), jnp.bfloat16)],
        compiler_params=params(),
        cost_estimate=pl.CostEstimate(
            flops=2 * outs * count * 9 * channels, bytes_accessed=18 * outs * channels, transcendentals=0
        ),
    )(*operands)


def gate_call(edges, own, pair, total, cell, cols):
    outs, count = total.shape
    channels = own.shape[3]
    width = 2 * cell.shape[1]
    tap = pl.BlockSpec((1, 3) + own.shape[2:], lambda i: (2 * i, 0, 0, 0))
    edge = constant((1,) + edges[0].shape[1:])
    return pl.pallas_call(
        functools.partial(gate_kernel, cols),
        grid=(2,),
        in_specs=[edge, edge, tap, tap, constant(total.shape), constant(cell.shape)],
        out_specs=[constant((count, width)), constant(cell.shape)],
        out_shape=[
            jax.ShapeDtypeStruct((count, width), jnp.bfloat16),
            jax.ShapeDtypeStruct(cell.shape, jnp.float32),
        ],
        scratch_shapes=[
            pltpu.VMEM((3, 4 * cols, channels), jnp.bfloat16),
            pltpu.VMEM((width, count), jnp.float32),
            pltpu.VMEM((outs, count), jnp.float32),
        ],
        compiler_params=params(),
        cost_estimate=pl.CostEstimate(
            flops=2 * outs * cols * 2 * 6 * channels, bytes_accessed=12 * outs * channels, transcendentals=0
        ),
    )(edges[0], edges[1], own, pair, total, cell)


def decoder_call(parts, edges, first, first_bias, second, second_bias, rows, width, margin, inner):
    groups = len(parts)
    channels = first.shape[2]
    outs = second.shape[3]
    return pl.pallas_call(
        functools.partial(decoder_kernel, groups, rows, width, margin, inner),
        grid=(6,),
        in_specs=[constant(part.shape) for part in parts]
        + [constant(edges[0].shape)] * 2
        + [
            pl.BlockSpec((1, 3) + first.shape[2:], lambda i: (jnp.minimum(i, 2), 0, 0, 0)),
            constant((1, first.shape[3])),
            pl.BlockSpec((1, 3) + second.shape[2:], lambda i: (jnp.maximum(i - 3, 0), 0, 0, 0)),
            constant((1, outs)),
        ],
        out_specs=constant((rows * width, outs)),
        out_shape=jax.ShapeDtypeStruct((rows * width, outs), jnp.bfloat16),
        scratch_shapes=[
            pltpu.VMEM((3, (rows + 4) * width, channels), jnp.bfloat16),
            pltpu.VMEM((3, (rows + 2) * width, first.shape[3]), jnp.bfloat16),
            pltpu.VMEM(((rows + 2) * width, first.shape[3]), jnp.float32),
            pltpu.VMEM((rows * width, outs), jnp.float32),
        ],
        compiler_params=params(),
        cost_estimate=pl.CostEstimate(
            flops=2 * 9 * channels * outs * (2 * rows + 2) * width,
            bytes_accessed=36 * channels * outs,
            transcendentals=0,
        ),
    )(*parts, *edges, first, first_bias.reshape(1, -1), second, second_bias.reshape(1, -1))


def per_device(
    frames,
    hidden_start,
    cell_start,
    input_weight,
    hidden_weight,
    gate_bias,
    first_weight,
    first_bias,
    second_weight,
    second_bias,
):
    steps, batch, rows, cols, share = frames.shape
    groups = lax.axis_size("hid") // 2
    patches = lax.axis_size("patch")
    assert batch == 2 and groups & (groups - 1) == 0 and patches % 2 == 0
    hid = lax.axis_index("hid")
    core = lax.rem(hid, 2)
    group = hid // 2
    even = lax.rem(lax.axis_index("patch"), 2) == 0
    count = rows * cols
    width = 2 * share

    pairs = [(i, i ^ 1) for i in range(2 * groups)]
    inner_pairs = [(i, i ^ 1) for i in range(patches)]
    outer_pairs = [(i, (i - 1) % patches if i % 2 == 0 else (i + 1) % patches) for i in range(patches)]

    def swap(value):
        return lax.ppermute(value, "hid", pairs)

    def own_batch(value, axis):
        mine = lax.dynamic_index_in_dim(value, core, axis, keepdims=False)
        other = lax.dynamic_index_in_dim(value, 1 - core, axis, keepdims=False)
        return mine, swap(other)

    def joined(value, axis):
        mine, other = own_batch(value, axis)
        return jnp.where(core == 0, jnp.concatenate([mine, other], -1), jnp.concatenate([other, mine], -1))

    def gathered(value):
        return [value] + [
            lax.ppermute(value, "hid", [(i, i ^ (2 * k)) for i in range(2 * groups)]) for k in range(1, groups)
        ]

    def swapped_edges(top, bottom):
        first = lax.ppermute(jnp.where(even, bottom, top), "patch", inner_pairs)
        second = lax.ppermute(jnp.where(even, top, bottom), "patch", outer_pairs)
        return first, second

    def edges_of(parts):
        top = jnp.stack([part[:, :cols] for part in parts], 1)
        bottom = jnp.stack([part[:, count - cols :] for part in parts], 1)
        return swapped_edges(top, bottom)

    def gate_major(weight):
        turned = jnp.transpose(weight, (0, 1, 3, 4, 2))
        return turned.reshape(turned.shape[:2] + (-1,) + turned.shape[-1:])

    hidden = joined(hidden_start, 0).reshape(1, count, width)
    images = joined(frames, 1).reshape(steps, count, width)
    input_own, hidden_own = gate_major(input_weight), gate_major(hidden_weight)
    lead = jnp.concatenate([images[:1], hidden], 0)
    lead_parts = gathered(lead)
    input_pair, hidden_pair = swap(input_own), swap(hidden_own)
    bias_own = gate_bias.reshape(-1)
    bias = jnp.concatenate([bias_own, swap(bias_own)]).reshape(-1, 1)
    cell_mine, cell_other = own_batch(cell_start, 0)
    cell = jnp.stack([cell_mine.reshape(count, share).T, cell_other.reshape(count, share).T])
    lead_edges = edges_of(lead_parts)

    rest, lead_edges = lax.optimization_barrier((images[1:], lead_edges))
    rest_parts = gathered(rest)
    rest_edges = edges_of(rest_parts)

    for time_index in range(steps):
        if time_index == 0:
            total = conv_call(lead_parts, 0, lead_edges, input_own, input_pair, bias, cols)
            parts, part_index = lead_parts, 1
            edges = tuple(edge[1:2] for edge in lead_edges)
        else:
            total = conv_call(rest_parts, time_index - 1, rest_edges, input_own, input_pair, bias, cols)
            parts, part_index = gathered(hidden[None]), 0
            edges = edges_of(parts)
        total = conv_call(parts, part_index, None, hidden_own, hidden_pair, total, cols)
        hidden, cell = gate_call(edges, hidden_own, hidden_pair, total, cell, cols)

    inner = cols // groups
    tile = -(-(inner + 4) // 16) * 16
    margin = (tile - inner) // 2
    image = jnp.pad(hidden.reshape(rows, cols, width), ((0, 0), (margin, margin), (0, 0)))

    def columns_for(k):
        start = lax.bitwise_xor(group, k) * inner
        return lax.dynamic_slice_in_dim(image, start, tile, axis=1).reshape(rows * tile, width)

    tiles = [columns_for(0)] + [
        lax.ppermute(columns_for(k), "hid", [(i, i ^ (2 * k)) for i in range(2 * groups)]) for k in range(1, groups)
    ]
    rim = 2 * tile
    tile_edges = swapped_edges(
        jnp.stack([part[:rim] for part in tiles])[None],
        jnp.stack([part[rows * tile - rim :] for part in tiles])[None],
    )
    decoded = decoder_call(
        tiles, tile_edges, first_weight, first_bias, second_weight, second_bias, rows, tile, margin, inner
    )
    decoded = decoded.reshape(rows, tile, -1)
    half = inner // 2
    mine = lax.dynamic_slice_in_dim(decoded, margin + core * half, half, axis=1)
    other = swap(lax.dynamic_slice_in_dim(decoded, margin + (1 - core) * half, half, axis=1))
    decoded = jnp.where(core == 0, jnp.stack([mine, other]), jnp.stack([other, mine]))

    cell_mine = cell[0].T.reshape(rows, cols, share)
    cell_other = swap(cell[1]).T.reshape(rows, cols, share)
    cell_final = jnp.where(core == 0, jnp.stack([cell_mine, cell_other]), jnp.stack([cell_other, cell_mine]))
    return decoded, cell_final


def solution(mesh):
    return jax.shard_map(
        per_device,
        mesh=mesh,
        in_specs=(
            P(None, None, "patch", None, "hid"),
            P(None, "patch", None, "hid"),
            P(None, "patch", None, "hid"),
            P(None, None, None, None, "hid"),
            P(None, None, None, None, "hid"),
            P(None, "hid"),
            P(),
            P(),
            P(),
            P(),
        ),
        out_specs=(P(None, "patch", "hid", None), P(None, "patch", None, "hid")),
        check_vma=False,
    )
```

```python
import functools

import jax
import jax.numpy as jnp
from jax import lax
from jax.experimental import pallas as pl
from jax.experimental.pallas import tpu as pltpu
from jax.sharding import PartitionSpec as P


FORGET_BIAS = 1.0
VMEM_LIMIT = 14 * 1024 * 1024

NT = (((1,), (1,)), ((), ()))
NN = (((1,), (0,)), ((), ()))


def place_columns(dst, row0, pieces, group, cols, masked):
    count, width = pieces[0].shape
    groups = len(pieces)
    place = lax.rem(lax.broadcasted_iota(jnp.int32, (count, width), 0), cols)

    def shifts(piece):
        wide = piece.astype(jnp.float32)
        low = pltpu.roll(wide, 1, 0)
        high = pltpu.roll(wide, count - 1, 0)
        if masked:
            low = jnp.where(place == 0, 0.0, low)
            high = jnp.where(place == cols - 1, 0.0, high)
        return (low.astype(dst.dtype), wide.astype(dst.dtype), high.astype(dst.dtype))

    shifted = [shifts(piece) for piece in pieces]
    rows = pl.ds(row0, count)
    if width % 128 == 0:
        for k in range(groups):
            lanes = pl.ds(pl.multiple_of(lax.bitwise_xor(group, k) * width, width), width)
            for q in range(3):
                dst[q, rows, lanes] = shifted[k][q]
    else:
        for j in range(groups):

            @pl.when(group == j)
            def _():
                for q in range(3):
                    dst[q, rows, :] = jnp.concatenate(
                        [shifted[j ^ i][q] for i in range(groups)], axis=1
                    )


def halo_pieces(a_ref, b_ref):
    patch = lax.axis_index("patch")
    even = lax.rem(patch, 2) == 0
    above = patch > 0
    below = patch < lax.axis_size("patch") - 1
    top, bottom = [], []
    for k in range(a_ref.shape[1]):
        a = a_ref[0, k].astype(jnp.float32)
        b = b_ref[0, k].astype(jnp.float32)
        top.append(jnp.where(above, jnp.where(even, b, a), 0.0))
        bottom.append(jnp.where(below, jnp.where(even, a, b), 0.0))
    return top, bottom


def conv_kernel(groups, cols, halo, *refs):
    refs = list(refs)
    parts = [refs.pop(0) for _ in range(groups)]
    if halo:
        edge_a, edge_b = refs.pop(0), refs.pop(0)
    own_ref, pair_ref, init_ref, out_ref, held = refs
    count = out_ref.shape[1]
    step = pl.program_id(0)
    group = lax.axis_index("hid") // 2

    @pl.when(step == 0)
    def _():
        place_columns(held, cols, [part[0] for part in parts], group, cols, True)
        if halo:
            top, bottom = halo_pieces(edge_a, edge_b)
            place_columns(held, 0, top, group, cols, True)
            place_columns(held, cols + count, bottom, group, cols, True)
        else:
            zero = jnp.zeros((cols, held.shape[2]), held.dtype)
            for q in range(3):
                held[q, pl.ds(0, cols), :] = zero
                held[q, pl.ds(cols + count, cols), :] = zero
        out_ref[...] = jnp.broadcast_to(init_ref[...], out_ref.shape)

    total = out_ref[...]
    for q in range(3):
        window = held[q, pl.ds(pl.multiple_of(step * cols, cols), count), :]
        weight = jnp.concatenate([own_ref[0, q], pair_ref[0, q]], axis=0)
        total = total + lax.dot_general(weight, window, NT, preferred_element_type=jnp.float32)
    out_ref[...] = total


def gate_kernel(cols, edge_a, edge_b, own_ref, pair_ref, total_ref, cell_ref, hidden_ref, cell_out, held, turned, summed):
    step = pl.program_id(0)
    group = lax.axis_index("hid") // 2
    core = lax.rem(lax.axis_index("hid"), 2)
    count = total_ref.shape[1]
    channels = cell_ref.shape[1]
    side = 2 * cols

    @pl.when(step == 0)
    def _():
        top, bottom = halo_pieces(edge_a, edge_b)
        zero = jnp.zeros((cols, held.shape[2]), held.dtype)
        for q in range(3):
            held[q, pl.ds(cols, cols), :] = zero
            held[q, pl.ds(2 * cols, cols), :] = zero
        place_columns(held, 0, top, group, cols, True)
        place_columns(held, 3 * cols, bottom, group, cols, True)
        summed[...] = total_ref[...]

    def add(row0, lane0):
        total = summed[:, lane0 : lane0 + side]
        for q in range(3):
            window = held[q, row0 : row0 + side, :]
            weight = jnp.concatenate([own_ref[0, q], pair_ref[0, q]], axis=0)
            total = total + lax.dot_general(weight, window, NT, preferred_element_type=jnp.float32)
        summed[:, lane0 : lane0 + side] = total

    @pl.when(step == 0)
    def _():
        add(0, 0)

    @pl.when(step == 1)
    def _():
        add(side, count - side)
        for half in range(2):
            base = half * 4 * channels
            z0, z1, z2, z3 = (summed[base + i * channels : base + (i + 1) * channels, :] for i in range(4))
            cell = jax.nn.sigmoid(z1 + FORGET_BIAS) * cell_ref[half] + jax.nn.sigmoid(z0) * jnp.tanh(z2)
            cell_out[half] = cell
            rows = pl.ds(pl.multiple_of(lax.bitwise_xor(core, half) * channels, channels), channels)
            turned[rows, :] = jax.nn.sigmoid(z3) * jnp.tanh(cell)
        hidden_ref[...] = turned[...].T.astype(hidden_ref.dtype)


def decoder_kernel(groups, rows, width, margin, inner, *refs):
    parts = refs[:groups]
    edge_a, edge_b, first_ref, bias1_ref, second_ref, bias2_ref, out_ref, held, middle, total1, total2 = refs[groups:]
    step = pl.program_id(0)
    hid = lax.axis_index("hid")
    group = hid // 2
    patch = lax.axis_index("patch")
    image_rows = rows * lax.axis_size("patch")
    image_cols = inner * groups

    @pl.when(step == 0)
    def _():
        top, bottom = halo_pieces(edge_a, edge_b)
        place_columns(held, 0, top, group, width, False)
        place_columns(held, 2 * width, [part[...] for part in parts], group, width, False)
        place_columns(held, (2 + rows) * width, bottom, group, width, False)
        total1[...] = jnp.broadcast_to(bias1_ref[...], total1.shape)

    @pl.when(step < 3)
    def _():
        total = total1[...]
        for q in range(3):
            window = held[q, pl.ds(pl.multiple_of(step * width, width), (rows + 2) * width), :]
            total = total + lax.dot_general(window, first_ref[0, q], NN, preferred_element_type=jnp.float32)
        total1[...] = total

    @pl.when(step == 3)
    def _():
        value = total1[...]
        place = lax.broadcasted_iota(jnp.int32, value.shape, 0)
        row = patch * rows + place // width - 1
        col = group * inner - margin + lax.rem(place, width)
        inside = (row >= 0) & (row < image_rows) & (col >= 0) & (col < image_cols)
        value = jnp.where(inside, value * jax.nn.sigmoid(value), 0.0)
        value = value.astype(middle.dtype).astype(jnp.float32)
        count = value.shape[0]
        middle[0] = pltpu.roll(value, 1, 0).astype(middle.dtype)
        middle[1] = value.astype(middle.dtype)
        middle[2] = pltpu.roll(value, count - 1, 0).astype(middle.dtype)
        total2[...] = jnp.broadcast_to(bias2_ref[...], total2.shape)

    @pl.when(step >= 3)
    def _():
        total = total2[...]
        for q in range(3):
            window = middle[q, pl.ds(pl.multiple_of((step - 3) * width, width), rows * width), :]
            total = total + lax.dot_general(window, second_ref[0, q], NN, preferred_element_type=jnp.float32)
        total2[...] = total

        @pl.when(step == 5)
        def _():
            out_ref[...] = total.astype(out_ref.dtype)


def constant(shape, index=None):
    index = (0,) * len(shape) if index is None else index
    return pl.BlockSpec(shape, lambda i: index)


def params():
    return pltpu.CompilerParams(vmem_limit_bytes=VMEM_LIMIT, dimension_semantics=("arbitrary",))


def conv_call(parts, index, edges, own, pair, init, cols):
    groups = len(parts)
    _, count, width = parts[0].shape
    channels = own.shape[3]
    outs = 2 * own.shape[2]
    tap = pl.BlockSpec((1, 3) + own.shape[2:], lambda i: (i, 0, 0, 0))
    specs = [constant((1, count, width), (index, 0, 0))] * groups
    operands = list(parts)
    if edges is not None:
        specs += [constant((1,) + edges[0].shape[1:], (index, 0, 0, 0))] * 2
        operands += list(edges)
    specs += [tap, tap, constant(init.shape)]
    if edges is not None:
        own, pair = (pltpu.with_memory_space_constraint(weight, pltpu.HBM) for weight in (own, pair))
    operands += [own, pair, init]
    return pl.pallas_call(
        functools.partial(conv_kernel, groups, cols, edges is not None),
        grid=(3,),
        in_specs=specs,
        out_specs=constant((outs, count)),
        out_shape=jax.ShapeDtypeStruct((outs, count), jnp.float32),
        scratch_shapes=[pltpu.VMEM((3, count + 2 * cols, channels), jnp.bfloat16)],
        compiler_params=params(),
        cost_estimate=pl.CostEstimate(
            flops=2 * outs * count * 9 * channels, bytes_accessed=18 * outs * channels, transcendentals=0
        ),
    )(*operands)


def gate_call(edges, own, pair, total, cell, cols):
    outs, count = total.shape
    channels = own.shape[3]
    width = 2 * cell.shape[1]
    tap = pl.BlockSpec((1, 3) + own.shape[2:], lambda i: (2 * i, 0, 0, 0))
    edge = constant((1,) + edges[0].shape[1:])
    return pl.pallas_call(
        functools.partial(gate_kernel, cols),
        grid=(2,),
        in_specs=[edge, edge, tap, tap, constant(total.shape), constant(cell.shape)],
        out_specs=[constant((count, width)), constant(cell.shape)],
        out_shape=[
            jax.ShapeDtypeStruct((count, width), jnp.bfloat16),
            jax.ShapeDtypeStruct(cell.shape, jnp.float32),
        ],
        scratch_shapes=[
            pltpu.VMEM((3, 4 * cols, channels), jnp.bfloat16),
            pltpu.VMEM((width, count), jnp.float32),
            pltpu.VMEM((outs, count), jnp.float32),
        ],
        compiler_params=params(),
        cost_estimate=pl.CostEstimate(
            flops=2 * outs * cols * 2 * 6 * channels, bytes_accessed=12 * outs * channels, transcendentals=0
        ),
    )(edges[0], edges[1], own, pair, total, cell)


def decoder_call(parts, edges, first, first_bias, second, second_bias, rows, width, margin, inner):
    groups = len(parts)
    channels = first.shape[2]
    outs = second.shape[3]
    return pl.pallas_call(
        functools.partial(decoder_kernel, groups, rows, width, margin, inner),
        grid=(6,),
        in_specs=[constant(part.shape) for part in parts]
        + [constant(edges[0].shape)] * 2
        + [
            pl.BlockSpec((1, 3) + first.shape[2:], lambda i: (jnp.minimum(i, 2), 0, 0, 0)),
            constant((1, first.shape[3])),
            pl.BlockSpec((1, 3) + second.shape[2:], lambda i: (jnp.maximum(i - 3, 0), 0, 0, 0)),
            constant((1, outs)),
        ],
        out_specs=constant((rows * width, outs)),
        out_shape=jax.ShapeDtypeStruct((rows * width, outs), jnp.bfloat16),
        scratch_shapes=[
            pltpu.VMEM((3, (rows + 4) * width, channels), jnp.bfloat16),
            pltpu.VMEM((3, (rows + 2) * width, first.shape[3]), jnp.bfloat16),
            pltpu.VMEM(((rows + 2) * width, first.shape[3]), jnp.float32),
            pltpu.VMEM((rows * width, outs), jnp.float32),
        ],
        compiler_params=params(),
        cost_estimate=pl.CostEstimate(
            flops=2 * 9 * channels * outs * (2 * rows + 2) * width,
            bytes_accessed=36 * channels * outs,
            transcendentals=0,
        ),
    )(
        *parts,
        *edges,
        pltpu.with_memory_space_constraint(first, pltpu.HBM),
        first_bias.reshape(1, -1),
        pltpu.with_memory_space_constraint(second, pltpu.HBM),
        second_bias.reshape(1, -1),
    )


def program(
    frames,
    hidden_start,
    cell_start,
    input_weight,
    hidden_weight,
    gate_bias,
    first_weight,
    first_bias,
    second_weight,
    second_bias,
):
    steps, batch, rows, cols, share = frames.shape
    groups = lax.axis_size("hid") // 2
    patches = lax.axis_size("patch")
    assert batch == 2 and groups & (groups - 1) == 0 and patches % 2 == 0
    hid = lax.axis_index("hid")
    core = lax.rem(hid, 2)
    group = hid // 2
    even = lax.rem(lax.axis_index("patch"), 2) == 0
    count = rows * cols
    width = 2 * share

    pairs = [(i, i ^ 1) for i in range(2 * groups)]
    inner_pairs = [(i, i ^ 1) for i in range(patches)]
    outer_pairs = [(i, (i - 1) % patches if i % 2 == 0 else (i + 1) % patches) for i in range(patches)]

    def swap(value):
        return lax.ppermute(value, "hid", pairs)

    def own_batch(value, axis):
        mine = lax.dynamic_index_in_dim(value, core, axis, keepdims=False)
        other = lax.dynamic_index_in_dim(value, 1 - core, axis, keepdims=False)
        return mine, swap(other)

    def joined(value, axis):
        mine, other = own_batch(value, axis)
        return jnp.where(core == 0, jnp.concatenate([mine, other], -1), jnp.concatenate([other, mine], -1))

    def gathered(value):
        return [value] + [
            lax.ppermute(value, "hid", [(i, i ^ (2 * k)) for i in range(2 * groups)]) for k in range(1, groups)
        ]

    def swapped_edges(top, bottom):
        first = lax.ppermute(jnp.where(even, bottom, top), "patch", inner_pairs)
        second = lax.ppermute(jnp.where(even, top, bottom), "patch", outer_pairs)
        return first, second

    def edges_of(parts):
        top = jnp.stack([part[:, :cols] for part in parts], 1)
        bottom = jnp.stack([part[:, count - cols :] for part in parts], 1)
        return swapped_edges(top, bottom)

    def gate_major(weight):
        turned = jnp.transpose(weight, (0, 1, 3, 4, 2))
        return turned.reshape(turned.shape[:2] + (-1,) + turned.shape[-1:])

    def ordered(mine, other, axis):
        return jnp.where(core == 0, jnp.concatenate([mine, other], axis), jnp.concatenate([other, mine], axis))

    def of_batch(index):
        return jnp.stack(
            [
                lax.dynamic_index_in_dim(frames[0], index, 0, keepdims=False),
                lax.dynamic_index_in_dim(hidden_start, index, 0, keepdims=False),
            ]
        )

    lead = ordered(of_batch(core), swap(of_batch(1 - core)), -1).reshape(2, count, width)
    lead, frames, cell_start, gate_bias = lax.optimization_barrier((lead, frames, cell_start, gate_bias))
    lead_parts = gathered(lead)
    rest = joined(frames[1:], 1).reshape(steps - 1, count, width)
    cell_mine, cell_other = own_batch(cell_start, 0)
    cell = jnp.stack([cell_mine.reshape(count, share).T, cell_other.reshape(count, share).T])
    bias_own = gate_bias.reshape(-1)
    bias = jnp.concatenate([bias_own, swap(bias_own)]).reshape(-1, 1)

    lead_parts, rest, cell, bias, input_own, hidden_own = lax.optimization_barrier(
        (lead_parts, rest, cell, bias, gate_major(input_weight), gate_major(hidden_weight))
    )
    input_pair, hidden_pair = swap(input_own), swap(hidden_own)
    lead_edges = edges_of(lead_parts)
    rest_parts = gathered(rest)
    rest_edges = edges_of(rest_parts)

    for time_index in range(steps):
        if time_index == 0:
            total = conv_call(lead_parts, 0, lead_edges, input_own, input_pair, bias, cols)
            parts, part_index = lead_parts, 1
            edges = tuple(edge[1:2] for edge in lead_edges)
        else:
            total = conv_call(rest_parts, time_index - 1, rest_edges, input_own, input_pair, bias, cols)
            parts, part_index = gathered(hidden[None]), 0
            edges = edges_of(parts)
        total = conv_call(parts, part_index, None, hidden_own, hidden_pair, total, cols)
        hidden, cell = gate_call(edges, hidden_own, hidden_pair, total, cell, cols)

    inner = cols // groups
    tile = -(-(inner + 4) // 16) * 16
    margin = (tile - inner) // 2
    image = jnp.pad(hidden.reshape(rows, cols, width), ((0, 0), (margin, margin), (0, 0)))

    def columns_for(k):
        start = lax.bitwise_xor(group, k) * inner
        return lax.dynamic_slice_in_dim(image, start, tile, axis=1).reshape(rows * tile, width)

    tiles = [columns_for(0)] + [
        lax.ppermute(columns_for(k), "hid", [(i, i ^ (2 * k)) for i in range(2 * groups)]) for k in range(1, groups)
    ]
    rim = 2 * tile
    tile_edges = swapped_edges(
        jnp.stack([part[:rim] for part in tiles])[None],
        jnp.stack([part[rows * tile - rim :] for part in tiles])[None],
    )
    decoded = decoder_call(
        tiles, tile_edges, first_weight, first_bias, second_weight, second_bias, rows, tile, margin, inner
    )
    decoded = decoded.reshape(rows, tile, -1)
    half = inner // 2
    mine = lax.dynamic_slice_in_dim(decoded, margin + core * half, half, axis=1)
    other = swap(lax.dynamic_slice_in_dim(decoded, margin + (1 - core) * half, half, axis=1))
    decoded = jnp.where(core == 0, jnp.stack([mine, other]), jnp.stack([other, mine]))

    cell_mine = cell[0].T.reshape(rows, cols, share)
    cell_other = swap(cell[1]).T.reshape(rows, cols, share)
    cell_final = jnp.where(core == 0, jnp.stack([cell_mine, cell_other]), jnp.stack([cell_other, cell_mine]))
    return decoded, cell_final


def solution(mesh):
    return jax.shard_map(
        program,
        mesh=mesh,
        in_specs=(
            P(None, None, "patch", None, "hid"),
            P(None, "patch", None, "hid"),
            P(None, "patch", None, "hid"),
            P(None, None, None, None, "hid"),
            P(None, None, None, None, "hid"),
            P(None, "hid"),
            P(),
            P(),
            P(),
            P(),
        ),
        out_specs=(P(None, "patch", "hid", None), P(None, "patch", None, "hid")),
        check_vma=False,
    )
```

```python
import functools

import jax
import jax.numpy as jnp
from jax import lax
from jax.experimental import pallas as pl
from jax.experimental.pallas import tpu as pltpu
from jax.sharding import PartitionSpec as P


FORGET_BIAS = 1.0
NT = (((1,), (1,)), ((), ()))
NN = (((1,), (0,)), ((), ()))


def place_columns(dst, row0, pieces, group, cols, masked):
    count, width = pieces[0].shape
    groups = len(pieces)
    place = lax.rem(lax.broadcasted_iota(jnp.int32, (count, width), 0), cols)

    def shifts(piece):
        wide = piece.astype(jnp.float32)
        low = pltpu.roll(wide, 1, 0)
        high = pltpu.roll(wide, count - 1, 0)
        if masked:
            low = jnp.where(place == 0, 0.0, low)
            high = jnp.where(place == cols - 1, 0.0, high)
        return (low.astype(dst.dtype), wide.astype(dst.dtype), high.astype(dst.dtype))

    shifted = [shifts(piece) for piece in pieces]
    rows = pl.ds(row0, count)
    if width % 128 == 0:
        for k in range(groups):
            lanes = pl.ds(pl.multiple_of(lax.bitwise_xor(group, k) * width, width), width)
            for q in range(3):
                dst[q, rows, lanes] = shifted[k][q]
    else:
        for j in range(groups):

            @pl.when(group == j)
            def _():
                for q in range(3):
                    dst[q, rows, :] = jnp.concatenate(
                        [shifted[j ^ i][q] for i in range(groups)], axis=1
                    )


def halo_pieces(a_ref, b_ref, index):
    patch = lax.axis_index("patch")
    even = lax.rem(patch, 2) == 0
    above = patch > 0
    below = patch < lax.axis_size("patch") - 1
    top, bottom = [], []
    for k in range(a_ref.shape[1]):
        a = a_ref[index, k].astype(jnp.float32)
        b = b_ref[index, k].astype(jnp.float32)
        top.append(jnp.where(above, jnp.where(even, b, a), 0.0))
        bottom.append(jnp.where(below, jnp.where(even, a, b), 0.0))
    return top, bottom


def stage_kernel(*refs):
    sources, target, semaphores = refs[:-2], refs[-2], refs[-1]
    copies = []
    for p in range(3):
        for q in range(3):
            for i, source in enumerate(sources):
                copy = pltpu.make_async_copy(source.at[p, q], target.at[p, q, i], semaphores.at[p, q, i])
                copy.start()
                copies.append(copy)
    for copy in copies:
        copy.wait()


def tap(weight_ref, p, q):
    weight = weight_ref[p, q]
    return weight.reshape(-1, weight.shape[-1])


def conv_kernel(groups, cols, index, halo, *refs):
    refs = list(refs)
    parts = [refs.pop(0) for _ in range(groups)]
    if halo:
        edge_a, edge_b = refs.pop(0), refs.pop(0)
    weight_ref, init_ref, out_ref, held = refs
    count = out_ref.shape[1]
    group = lax.axis_index("hid") // 2

    place_columns(held, cols, [part[index] for part in parts], group, cols, True)
    if halo:
        top, bottom = halo_pieces(edge_a, edge_b, index)
        place_columns(held, 0, top, group, cols, True)
        place_columns(held, cols + count, bottom, group, cols, True)
    else:
        zero = jnp.zeros((cols, held.shape[2]), held.dtype)
        for q in range(3):
            held[q, pl.ds(0, cols), :] = zero
            held[q, pl.ds(cols + count, cols), :] = zero
    if init_ref.shape == out_ref.shape:
        total = init_ref[...]
    else:
        column = jnp.broadcast_to(init_ref[...], (8, out_ref.shape[0])).T
        total = jnp.broadcast_to(column[:, :1], out_ref.shape)
    for p in range(3):
        for q in range(3):
            window = held[q, p * cols : p * cols + count, :]
            total = total + lax.dot_general(
                tap(weight_ref, p, q), window, NT, preferred_element_type=jnp.float32
            )
    out_ref[...] = total


def gate_kernel(cols, indices, turn_in, turn_out, *refs):
    refs = list(refs)
    sides = [(refs.pop(0), refs.pop(0), refs.pop(0), index) for index in indices]
    total_ref = refs.pop(0)
    cells = [refs.pop(0), refs.pop(0)]
    hidden_ref = refs.pop(0)
    cells_out = [refs.pop(0), refs.pop(0)]
    held, turned, summed = refs
    group = lax.axis_index("hid") // 2
    core = lax.rem(lax.axis_index("hid"), 2)
    count = total_ref.shape[1]
    channels = total_ref.shape[0] // 8
    side = 2 * cols

    summed[...] = total_ref[...]
    zero = jnp.zeros((cols, held.shape[2]), held.dtype)
    for q in range(3):
        held[q, pl.ds(cols, cols), :] = zero
        held[q, pl.ds(2 * cols, cols), :] = zero
    for edge_a, edge_b, weight_ref, index in sides:
        top, bottom = halo_pieces(edge_a, edge_b, index)
        place_columns(held, 0, top, group, cols, True)
        place_columns(held, 3 * cols, bottom, group, cols, True)
        for p, row0, lane0 in ((0, 0, 0), (2, side, count - side)):
            total = summed[:, lane0 : lane0 + side]
            for q in range(3):
                window = held[q, row0 : row0 + side, :]
                total = total + lax.dot_general(
                    tap(weight_ref, p, q), window, NT, preferred_element_type=jnp.float32
                )
            summed[:, lane0 : lane0 + side] = total
    for half in range(2):
        base = half * 4 * channels
        z0, z1, z2, z3 = (summed[base + i * channels : base + (i + 1) * channels, :] for i in range(4))
        cell = cells[half][...].T if turn_in else cells[half][...]
        cell = jax.nn.sigmoid(z1 + FORGET_BIAS) * cell + jax.nn.sigmoid(z0) * jnp.tanh(z2)
        cells_out[half][...] = cell.T if turn_out else cell
        rows = pl.ds(pl.multiple_of(lax.bitwise_xor(core, half) * channels, channels), channels)
        turned[rows, :] = jax.nn.sigmoid(z3) * jnp.tanh(cell)
    hidden_ref[0] = turned[...].T.astype(hidden_ref.dtype)


def decoder_kernel(groups, rows, width, margin, inner, *refs):
    parts = refs[:groups]
    edge_a, edge_b, first_ref, bias1_ref, second_ref, bias2_ref, out_ref, held, middle = refs[groups:]
    group = lax.axis_index("hid") // 2
    patch = lax.axis_index("patch")
    image_rows = rows * lax.axis_size("patch")
    image_cols = inner * groups

    def conv(source, weight_ref, bias_ref, count):
        total = jnp.broadcast_to(bias_ref[...], (count * width, bias_ref.shape[1]))
        for p in range(3):
            for q in range(3):
                window = source[q, p * width : (p + count) * width, :]
                total = total + lax.dot_general(
                    window, tap(weight_ref, p, q), NN, preferred_element_type=jnp.float32
                )
        return total

    top, bottom = halo_pieces(edge_a, edge_b, 0)
    place_columns(held, 0, top, group, width, False)
    place_columns(held, 2 * width, [part[...] for part in parts], group, width, False)
    place_columns(held, (2 + rows) * width, bottom, group, width, False)
    value = conv(held, first_ref, bias1_ref, rows + 2)
    place = lax.broadcasted_iota(jnp.int32, value.shape, 0)
    row = patch * rows + place // width - 1
    col = group * inner - margin + lax.rem(place, width)
    inside = (row >= 0) & (row < image_rows) & (col >= 0) & (col < image_cols)
    value = jnp.where(inside, value * jax.nn.sigmoid(value), 0.0)
    value = value.astype(middle.dtype).astype(jnp.float32)
    middle[0] = pltpu.roll(value, 1, 0).astype(middle.dtype)
    middle[1] = value.astype(middle.dtype)
    middle[2] = pltpu.roll(value, value.shape[0] - 1, 0).astype(middle.dtype)
    out_ref[...] = conv(middle, second_ref, bias2_ref, rows).astype(out_ref.dtype)


WHOLE = pl.BlockSpec(memory_space=pltpu.VMEM)
VMEM_LIMIT = 10 * 1024 * 1024


def params():
    return pltpu.CompilerParams(vmem_limit_bytes=VMEM_LIMIT)


def cost(flops, size):
    return pl.CostEstimate(flops=flops, bytes_accessed=size, transcendentals=0)


def stage_call(*sources):
    shape = sources[0].shape[:2] + (len(sources),) + sources[0].shape[2:]
    size = 2 * sources[0].size * len(sources)
    return pl.pallas_call(
        stage_kernel,
        in_specs=[pl.BlockSpec(memory_space=pltpu.HBM)] * len(sources),
        out_specs=WHOLE,
        out_shape=pltpu.VMEM(shape, sources[0].dtype),
        scratch_shapes=[pltpu.SemaphoreType.DMA((3, 3, len(sources)))],
        compiler_params=params(),
        cost_estimate=cost(100 * size, size),
    )(*(pltpu.with_memory_space_constraint(source, pltpu.HBM) for source in sources))


def conv_call(parts, index, edges, weight, init, cols):
    groups = len(parts)
    count = parts[0].shape[1]
    channels = weight.shape[-1]
    outs = 2 * weight.shape[3]
    operands = list(parts) + ([] if edges is None else list(edges)) + [weight, init]
    return pl.pallas_call(
        functools.partial(conv_kernel, groups, cols, index, edges is not None),
        in_specs=[WHOLE] * len(operands),
        out_specs=WHOLE,
        out_shape=jax.ShapeDtypeStruct((outs, count), jnp.float32),
        scratch_shapes=[pltpu.VMEM((3, count + 2 * cols, channels), jnp.bfloat16)],
        compiler_params=params(),
        cost_estimate=cost(2 * outs * count * 9 * channels, 18 * outs * channels),
    )(*operands)


def gate_call(sides, total, cells, cols, turn_in, turn_out):
    outs, count = total.shape
    channels = sides[0][2].shape[-1]
    share = outs // 8
    width = 2 * share
    cell_shape = (count, share) if turn_out else (share, count)
    operands = []
    for edges, _, weight in sides:
        operands += [edges[0], edges[1], weight]
    operands += [total, *cells]
    return pl.pallas_call(
        functools.partial(gate_kernel, cols, [index for _, index, _ in sides], turn_in, turn_out),
        in_specs=[WHOLE] * len(operands),
        out_specs=[WHOLE] * 3,
        out_shape=[jax.ShapeDtypeStruct((1, count, width), jnp.bfloat16)]
        + [jax.ShapeDtypeStruct(cell_shape, jnp.float32)] * 2,
        scratch_shapes=[
            pltpu.VMEM((3, 4 * cols, channels), jnp.bfloat16),
            pltpu.VMEM((width, count), jnp.float32),
            pltpu.VMEM((outs, count), jnp.float32),
        ],
        compiler_params=params(),
        cost_estimate=cost(2 * outs * count * 6 * channels, 12 * outs * channels),
    )(*operands)


def decoder_call(parts, edges, first, first_bias, second, second_bias, rows, width, margin, inner):
    groups = len(parts)
    channels = first.shape[3]
    outs = second.shape[4]
    operands = [*parts, *edges, first, first_bias.reshape(1, -1), second, second_bias.reshape(1, -1)]
    return pl.pallas_call(
        functools.partial(decoder_kernel, groups, rows, width, margin, inner),
        in_specs=[WHOLE] * len(operands),
        out_specs=WHOLE,
        out_shape=jax.ShapeDtypeStruct((rows * width, outs), jnp.bfloat16),
        scratch_shapes=[
            pltpu.VMEM((3, (rows + 4) * width, channels), jnp.bfloat16),
            pltpu.VMEM((3, (rows + 2) * width, first.shape[4]), jnp.bfloat16),
        ],
        compiler_params=params(),
        cost_estimate=cost(18 * channels * outs * (2 * rows + 2) * width, 36 * channels * outs),
    )(*operands)


def program(
    frames,
    hidden_start,
    cell_start,
    input_weight,
    hidden_weight,
    gate_bias,
    first_weight,
    first_bias,
    second_weight,
    second_bias,
):
    steps, batch, rows, cols, share = frames.shape
    groups = lax.axis_size("hid") // 2
    patches = lax.axis_size("patch")
    assert batch == 2 and groups & (groups - 1) == 0 and patches % 2 == 0
    hid = lax.axis_index("hid")
    core = lax.rem(hid, 2)
    group = hid // 2
    even = lax.rem(lax.axis_index("patch"), 2) == 0
    count = rows * cols
    width = 2 * share

    pairs = [(i, i ^ 1) for i in range(2 * groups)]
    inner_pairs = [(i, i ^ 1) for i in range(patches)]
    outer_pairs = [(i, (i - 1) % patches if i % 2 == 0 else (i + 1) % patches) for i in range(patches)]

    def swap(value):
        return lax.ppermute(value, "hid", pairs)

    def own_batch(value, axis):
        mine = lax.dynamic_index_in_dim(value, core, axis, keepdims=False, allow_negative_indices=False)
        other = lax.dynamic_index_in_dim(value, 1 - core, axis, keepdims=False, allow_negative_indices=False)
        return mine, swap(other)

    def joined(value, axis):
        mine, other = own_batch(value, axis)
        return jnp.where(core == 0, jnp.concatenate([mine, other], -1), jnp.concatenate([other, mine], -1))

    def gathered(value):
        return [value] + [
            lax.ppermute(value, "hid", [(i, i ^ (2 * k)) for i in range(2 * groups)]) for k in range(1, groups)
        ]

    def swapped_edges(top, bottom):
        first = lax.ppermute(jnp.where(even, bottom, top), "patch", inner_pairs)
        second = lax.ppermute(jnp.where(even, top, bottom), "patch", outer_pairs)
        return first, second

    def edges_of(parts):
        top = jnp.stack([part[:, :cols] for part in parts], 1)
        bottom = jnp.stack([part[:, count - cols :] for part in parts], 1)
        return swapped_edges(top, bottom)

    def gate_major(weight):
        turned = jnp.transpose(weight, (0, 1, 3, 4, 2))
        return turned.reshape(turned.shape[:2] + (-1,) + turned.shape[-1:])

    def ordered(mine, other, axis):
        return jnp.where(core == 0, jnp.concatenate([mine, other], axis), jnp.concatenate([other, mine], axis))

    def of_batch(index):
        return jnp.stack(
            [
                lax.dynamic_index_in_dim(frames[0], index, 0, keepdims=False, allow_negative_indices=False),
                lax.dynamic_index_in_dim(hidden_start, index, 0, keepdims=False, allow_negative_indices=False),
            ]
        )

    lead = ordered(of_batch(core), swap(of_batch(1 - core)), -1).reshape(2, count, width)
    inner = cols // groups
    tile = -(-(inner + 4) // 16) * 16
    margin = (tile - inner) // 2
    starts = [lax.bitwise_xor(group, k) * inner for k in range(groups)]
    out_starts = [margin + core * (inner // 2), margin + (1 - core) * (inner // 2)]
    (lead, starts, out_starts), frames, cell_start, gate_bias, input_own, hidden_own, first_weight, second_weight = (
        lax.optimization_barrier(
            (
                (lead, starts, out_starts),
                frames,
                cell_start,
                gate_bias,
                gate_major(input_weight),
                gate_major(hidden_weight),
                first_weight,
                second_weight,
            )
        )
    )
    lead_parts = gathered(lead)
    input_pair, hidden_pair = swap(input_own), swap(hidden_own)
    first_weight, second_weight = stage_call(first_weight), stage_call(second_weight)
    input_both = stage_call(input_own, input_pair)
    hidden_both = stage_call(hidden_own, hidden_pair)
    rest = joined(frames[1:], 1).reshape(steps - 1, count, width)
    cell_mine, cell_other = own_batch(cell_start, 0)
    cells = [cell_mine.reshape(count, share), cell_other.reshape(count, share)]
    bias_own = gate_bias.reshape(-1)
    bias = jnp.concatenate([bias_own, swap(bias_own)]).reshape(1, -1)

    lead_parts, rest, cells, bias = lax.optimization_barrier((lead_parts, rest, cells, bias))
    lead_edges = edges_of(lead_parts)
    rest_parts = gathered(rest)
    rest_edges = edges_of(rest_parts)

    for time_index in range(steps):
        if time_index == 0:
            total = conv_call(lead_parts, 0, None, input_both, bias, cols)
            parts, part_index, edges = lead_parts, 1, lead_edges
            sides = [(lead_edges, 0, input_both)]
        else:
            late = time_index > 1
            total = conv_call(
                rest_parts, time_index - 1, rest_edges if late else None, input_both, bias, cols
            )
            parts, part_index = gathered(hidden), 0
            edges = edges_of(parts)
            sides = [] if late else [(rest_edges, time_index - 1, input_both)]
        sides.append((edges, part_index, hidden_both))
        total = conv_call(parts, part_index, None, hidden_both, total, cols)
        hidden, *cells = gate_call(sides, total, cells, cols, time_index == 0, time_index == steps - 1)

    image = jnp.pad(hidden.reshape(rows, cols, width), ((0, 0), (margin, margin), (0, 0)))

    def columns_for(k):
        piece = lax.dynamic_slice_in_dim(image, starts[k], tile, axis=1, allow_negative_indices=False)
        return piece.reshape(rows * tile, width)

    tiles = [columns_for(0)] + [
        lax.ppermute(columns_for(k), "hid", [(i, i ^ (2 * k)) for i in range(2 * groups)]) for k in range(1, groups)
    ]
    rim = 2 * tile
    tile_edges = swapped_edges(
        jnp.stack([part[:rim] for part in tiles])[None],
        jnp.stack([part[rows * tile - rim :] for part in tiles])[None],
    )
    decoded = decoder_call(
        tiles, tile_edges, first_weight, first_bias, second_weight, second_bias, rows, tile, margin, inner
    )
    decoded = decoded.reshape(rows, tile, -1)
    mine, other = (
        lax.dynamic_slice_in_dim(decoded, start, inner // 2, axis=1, allow_negative_indices=False)
        for start in out_starts
    )
    other = swap(other)
    decoded = jnp.where(core == 0, jnp.stack([mine, other]), jnp.stack([other, mine]))

    cell_mine = cells[0].reshape(rows, cols, share)
    cell_other = swap(cells[1]).reshape(rows, cols, share)
    cell_final = jnp.where(core == 0, jnp.stack([cell_mine, cell_other]), jnp.stack([cell_other, cell_mine]))
    return decoded, cell_final


def solution(mesh):
    return jax.shard_map(
        program,
        mesh=mesh,
        in_specs=(
            P(None, None, "patch", None, "hid"),
            P(None, "patch", None, "hid"),
            P(None, "patch", None, "hid"),
            P(None, None, None, None, "hid"),
            P(None, None, None, None, "hid"),
            P(None, "hid"),
            P(),
            P(),
            P(),
            P(),
        ),
        out_specs=(P(None, "patch", "hid", None), P(None, "patch", None, "hid")),
        check_vma=False,
    )
```

```python
import functools

import jax
import jax.numpy as jnp
from jax import lax
from jax.experimental import pallas as pl
from jax.experimental.pallas import tpu as pltpu
from jax.sharding import PartitionSpec as P


FORGET_BIAS = 1.0
NT = (((1,), (1,)), ((), ()))
NN = (((1,), (0,)), ((), ()))


def place_columns(dst, row0, pieces, group, cols, masked):
    count, width = pieces[0].shape
    groups = len(pieces)
    place = lax.rem(lax.broadcasted_iota(jnp.int32, (count, width), 0), cols)

    def shifts(piece):
        wide = piece.astype(jnp.float32)
        low = pltpu.roll(wide, 1, 0)
        high = pltpu.roll(wide, count - 1, 0)
        if masked:
            low = jnp.where(place == 0, 0.0, low)
            high = jnp.where(place == cols - 1, 0.0, high)
        return (low.astype(dst.dtype), wide.astype(dst.dtype), high.astype(dst.dtype))

    shifted = [shifts(piece) for piece in pieces]
    rows = pl.ds(row0, count)
    if width % 128 == 0:
        for k in range(groups):
            lanes = pl.ds(pl.multiple_of(lax.bitwise_xor(group, k) * width, width), width)
            for q in range(3):
                dst[q, rows, lanes] = shifted[k][q]
    else:
        for j in range(groups):

            @pl.when(group == j)
            def _():
                for q in range(3):
                    dst[q, rows, :] = jnp.concatenate(
                        [shifted[j ^ i][q] for i in range(groups)], axis=1
                    )


def halo_pieces(a_ref, b_ref, index):
    patch = lax.axis_index("patch")
    even = lax.rem(patch, 2) == 0
    above = patch > 0
    below = patch < lax.axis_size("patch") - 1
    top, bottom = [], []
    for k in range(a_ref.shape[1]):
        a = a_ref[index, k].astype(jnp.float32)
        b = b_ref[index, k].astype(jnp.float32)
        top.append(jnp.where(above, jnp.where(even, b, a), 0.0))
        bottom.append(jnp.where(below, jnp.where(even, a, b), 0.0))
    return top, bottom


def stage_kernel(source, target, semaphores):
    copies = []
    for p in range(3):
        for q in range(3):
            copy = pltpu.make_async_copy(source.at[p, q], target.at[p, q], semaphores.at[p, q])
            copy.start()
            copies.append(copy)
    for copy in copies:
        copy.wait()


def tap(weight_refs, p, q):
    return jnp.concatenate([weight_ref[p, q] for weight_ref in weight_refs], axis=0)


def conv_kernel(groups, cols, index, halo, *refs):
    refs = list(refs)
    parts = [refs.pop(0) for _ in range(groups)]
    if halo:
        edge_a, edge_b = refs.pop(0), refs.pop(0)
    own_ref, pair_ref, init_ref, out_ref, held = refs
    count = out_ref.shape[1]
    group = lax.axis_index("hid") // 2

    place_columns(held, cols, [part[index] for part in parts], group, cols, True)
    if halo:
        top, bottom = halo_pieces(edge_a, edge_b, index)
        place_columns(held, 0, top, group, cols, True)
        place_columns(held, cols + count, bottom, group, cols, True)
    else:
        zero = jnp.zeros((cols, held.shape[2]), held.dtype)
        for q in range(3):
            held[q, pl.ds(0, cols), :] = zero
            held[q, pl.ds(cols + count, cols), :] = zero
    if init_ref.shape == out_ref.shape:
        total = init_ref[...]
    else:
        column = jnp.broadcast_to(init_ref[...], (8, out_ref.shape[0])).T
        total = jnp.broadcast_to(column[:, :1], out_ref.shape)
    for p in range(3):
        for q in range(3):
            window = held[q, p * cols : p * cols + count, :]
            total = total + lax.dot_general(
                tap((own_ref, pair_ref), p, q), window, NT, preferred_element_type=jnp.float32
            )
    out_ref[...] = total


def gate_kernel(cols, indices, turn_in, turn_out, *refs):
    refs = list(refs)
    sides = [(refs.pop(0), refs.pop(0), (refs.pop(0), refs.pop(0)), index) for index in indices]
    total_ref = refs.pop(0)
    cells = [refs.pop(0), refs.pop(0)]
    hidden_ref = refs.pop(0)
    cells_out = [refs.pop(0), refs.pop(0)]
    held, turned, summed = refs
    group = lax.axis_index("hid") // 2
    core = lax.rem(lax.axis_index("hid"), 2)
    count = total_ref.shape[1]
    channels = total_ref.shape[0] // 8
    side = 2 * cols

    summed[...] = total_ref[...]
    zero = jnp.zeros((cols, held.shape[2]), held.dtype)
    for q in range(3):
        held[q, pl.ds(cols, cols), :] = zero
        held[q, pl.ds(2 * cols, cols), :] = zero
    for edge_a, edge_b, weight_refs, index in sides:
        top, bottom = halo_pieces(edge_a, edge_b, index)
        place_columns(held, 0, top, group, cols, True)
        place_columns(held, 3 * cols, bottom, group, cols, True)
        for p, row0, lane0 in ((0, 0, 0), (2, side, count - side)):
            total = summed[:, lane0 : lane0 + side]
            for q in range(3):
                window = held[q, row0 : row0 + side, :]
                total = total + lax.dot_general(
                    tap(weight_refs, p, q), window, NT, preferred_element_type=jnp.float32
                )
            summed[:, lane0 : lane0 + side] = total
    for half in range(2):
        base = half * 4 * channels
        z0, z1, z2, z3 = (summed[base + i * channels : base + (i + 1) * channels, :] for i in range(4))
        cell = cells[half][...].T if turn_in else cells[half][...]
        cell = jax.nn.sigmoid(z1 + FORGET_BIAS) * cell + jax.nn.sigmoid(z0) * jnp.tanh(z2)
        cells_out[half][...] = cell.T if turn_out else cell
        rows = pl.ds(pl.multiple_of(lax.bitwise_xor(core, half) * channels, channels), channels)
        turned[rows, :] = jax.nn.sigmoid(z3) * jnp.tanh(cell)
    hidden_ref[0] = turned[...].T.astype(hidden_ref.dtype)


def decoder_kernel(groups, rows, width, margin, inner, *refs):
    parts = refs[:groups]
    edge_a, edge_b, first_ref, bias1_ref, second_ref, bias2_ref, out_ref, held, middle = refs[groups:]
    group = lax.axis_index("hid") // 2
    patch = lax.axis_index("patch")
    image_rows = rows * lax.axis_size("patch")
    image_cols = inner * groups

    def conv(source, weight_ref, bias_ref, count):
        total = jnp.broadcast_to(bias_ref[...], (count * width, bias_ref.shape[1]))
        for p in range(3):
            for q in range(3):
                window = source[q, p * width : (p + count) * width, :]
                total = total + lax.dot_general(
                    window, weight_ref[p, q], NN, preferred_element_type=jnp.float32
                )
        return total

    top, bottom = halo_pieces(edge_a, edge_b, 0)
    place_columns(held, 0, top, group, width, False)
    place_columns(held, 2 * width, [part[...] for part in parts], group, width, False)
    place_columns(held, (2 + rows) * width, bottom, group, width, False)
    value = conv(held, first_ref, bias1_ref, rows + 2)
    place = lax.broadcasted_iota(jnp.int32, value.shape, 0)
    row = patch * rows + place // width - 1
    col = group * inner - margin + lax.rem(place, width)
    inside = (row >= 0) & (row < image_rows) & (col >= 0) & (col < image_cols)
    value = jnp.where(inside, value * jax.nn.sigmoid(value), 0.0)
    value = value.astype(middle.dtype).astype(jnp.float32)
    middle[0] = pltpu.roll(value, 1, 0).astype(middle.dtype)
    middle[1] = value.astype(middle.dtype)
    middle[2] = pltpu.roll(value, value.shape[0] - 1, 0).astype(middle.dtype)
    out_ref[...] = conv(middle, second_ref, bias2_ref, rows).astype(out_ref.dtype)


WHOLE = pl.BlockSpec(memory_space=pltpu.VMEM)
VMEM_LIMIT = 10 * 1024 * 1024


def params():
    return pltpu.CompilerParams(vmem_limit_bytes=VMEM_LIMIT)


def cost(flops, size):
    return pl.CostEstimate(flops=flops, bytes_accessed=size, transcendentals=0)


def stage_call(source):
    size = 2 * source.size
    return pl.pallas_call(
        stage_kernel,
        in_specs=[pl.BlockSpec(memory_space=pltpu.HBM)],
        out_specs=WHOLE,
        out_shape=pltpu.VMEM(source.shape, source.dtype),
        scratch_shapes=[pltpu.SemaphoreType.DMA((3, 3))],
        compiler_params=params(),
        cost_estimate=cost(100 * size, size),
    )(pltpu.with_memory_space_constraint(source, pltpu.HBM))


def conv_call(parts, index, edges, weights, init, cols):
    groups = len(parts)
    count = parts[0].shape[1]
    channels = weights[0].shape[-1]
    outs = 2 * weights[0].shape[2]
    operands = list(parts) + ([] if edges is None else list(edges)) + [*weights, init]
    return pl.pallas_call(
        functools.partial(conv_kernel, groups, cols, index, edges is not None),
        in_specs=[WHOLE] * len(operands),
        out_specs=WHOLE,
        out_shape=jax.ShapeDtypeStruct((outs, count), jnp.float32),
        scratch_shapes=[pltpu.VMEM((3, count + 2 * cols, channels), jnp.bfloat16)],
        compiler_params=params(),
        cost_estimate=cost(2 * outs * count * 9 * channels, 18 * outs * channels),
    )(*operands)


def gate_call(sides, total, cells, cols, turn_in, turn_out):
    outs, count = total.shape
    channels = sides[0][2][0].shape[-1]
    share = outs // 8
    width = 2 * share
    cell_shape = (count, share) if turn_out else (share, count)
    operands = []
    for edges, _, weights in sides:
        operands += [*edges, *weights]
    operands += [total, *cells]
    return pl.pallas_call(
        functools.partial(gate_kernel, cols, [index for _, index, _ in sides], turn_in, turn_out),
        in_specs=[WHOLE] * len(operands),
        out_specs=[WHOLE] * 3,
        out_shape=[jax.ShapeDtypeStruct((1, count, width), jnp.bfloat16)]
        + [jax.ShapeDtypeStruct(cell_shape, jnp.float32)] * 2,
        scratch_shapes=[
            pltpu.VMEM((3, 4 * cols, channels), jnp.bfloat16),
            pltpu.VMEM((width, count), jnp.float32),
            pltpu.VMEM((outs, count), jnp.float32),
        ],
        compiler_params=params(),
        cost_estimate=cost(2 * outs * count * 6 * channels, 12 * outs * channels),
    )(*operands)


def decoder_call(parts, edges, first, first_bias, second, second_bias, rows, width, margin, inner):
    groups = len(parts)
    channels = first.shape[2]
    outs = second.shape[3]
    operands = [*parts, *edges, first, first_bias.reshape(1, -1), second, second_bias.reshape(1, -1)]
    return pl.pallas_call(
        functools.partial(decoder_kernel, groups, rows, width, margin, inner),
        in_specs=[WHOLE] * len(operands),
        out_specs=WHOLE,
        out_shape=jax.ShapeDtypeStruct((rows * width, outs), jnp.bfloat16),
        scratch_shapes=[
            pltpu.VMEM((3, (rows + 4) * width, channels), jnp.bfloat16),
            pltpu.VMEM((3, (rows + 2) * width, first.shape[3]), jnp.bfloat16),
        ],
        compiler_params=params(),
        cost_estimate=cost(18 * channels * outs * (2 * rows + 2) * width, 36 * channels * outs),
    )(*operands)


def program(
    frames,
    hidden_start,
    cell_start,
    input_weight,
    hidden_weight,
    gate_bias,
    first_weight,
    first_bias,
    second_weight,
    second_bias,
):
    steps, batch, rows, cols, share = frames.shape
    groups = lax.axis_size("hid") // 2
    patches = lax.axis_size("patch")
    assert batch == 2 and groups & (groups - 1) == 0 and patches % 2 == 0
    hid = lax.axis_index("hid")
    core = lax.rem(hid, 2)
    group = hid // 2
    even = lax.rem(lax.axis_index("patch"), 2) == 0
    count = rows * cols
    width = 2 * share

    pairs = [(i, i ^ 1) for i in range(2 * groups)]
    inner_pairs = [(i, i ^ 1) for i in range(patches)]
    outer_pairs = [(i, (i - 1) % patches if i % 2 == 0 else (i + 1) % patches) for i in range(patches)]

    def swap(value):
        return lax.ppermute(value, "hid", pairs)

    def own_batch(value, axis):
        mine = lax.dynamic_index_in_dim(value, core, axis, keepdims=False, allow_negative_indices=False)
        other = lax.dynamic_index_in_dim(value, 1 - core, axis, keepdims=False, allow_negative_indices=False)
        return mine, swap(other)

    def gathered(value):
        return [value] + [
            lax.ppermute(value, "hid", [(i, i ^ (2 * k)) for i in range(2 * groups)]) for k in range(1, groups)
        ]

    def swapped_edges(top, bottom):
        first = lax.ppermute(jnp.where(even, bottom, top), "patch", inner_pairs)
        second = lax.ppermute(jnp.where(even, top, bottom), "patch", outer_pairs)
        return first, second

    def edges_of(parts):
        top = jnp.stack([part[:, :cols] for part in parts], 1)
        bottom = jnp.stack([part[:, count - cols :] for part in parts], 1)
        return swapped_edges(top, bottom)

    def gate_major(weight):
        turned = jnp.transpose(weight, (0, 1, 3, 4, 2))
        return turned.reshape(turned.shape[:2] + (-1,) + turned.shape[-1:])

    def ordered(mine, other, axis):
        return jnp.where(core == 0, jnp.concatenate([mine, other], axis), jnp.concatenate([other, mine], axis))

    def frames_of(index, first):
        size = (steps - 1 if first else 1, 1) + frames.shape[2:]
        return lax.dynamic_slice(frames, (first, index, 0, 0, 0), size, allow_negative_indices=False)[:, 0]

    def of_batch(index):
        state = lax.dynamic_slice_in_dim(hidden_start, index, 1, 0, allow_negative_indices=False)
        return jnp.concatenate([frames_of(index, 0), state], 0)

    lead = ordered(of_batch(core), swap(of_batch(1 - core)), -1).reshape(2, count, width)
    inner = cols // groups
    tile = -(-(inner + 4) // 16) * 16
    margin = (tile - inner) // 2
    starts = [lax.bitwise_xor(group, k) * inner for k in range(groups)]
    out_starts = [margin + core * (inner // 2), margin + (1 - core) * (inner // 2)]
    (lead, starts, out_starts), frames, cell_start, gate_bias, input_own, hidden_own, first_weight, second_weight = (
        lax.optimization_barrier(
            (
                (lead, starts, out_starts),
                frames,
                cell_start,
                gate_bias,
                gate_major(input_weight),
                gate_major(hidden_weight),
                first_weight,
                second_weight,
            )
        )
    )
    lead_parts = gathered(lead)
    input_pair, hidden_pair = swap(input_own), swap(hidden_own)
    input_both, hidden_both = (input_own, input_pair), (hidden_own, hidden_pair)
    first_weight, second_weight = stage_call(first_weight), stage_call(second_weight)
    rest = ordered(frames_of(core, 1), swap(frames_of(1 - core, 1)), -1).reshape(steps - 1, count, width)
    cell_mine, cell_other = own_batch(cell_start, 0)
    cells = [cell_mine.reshape(count, share), cell_other.reshape(count, share)]
    bias_own = gate_bias.reshape(-1)
    bias = jnp.concatenate([bias_own, swap(bias_own)]).reshape(1, -1)

    lead_parts, cells, bias = lax.optimization_barrier((lead_parts, cells, bias))
    lead_edges = edges_of(lead_parts)
    rest_parts = gathered(rest)
    rest_edges = edges_of(rest_parts)

    for time_index in range(steps):
        if time_index == 0:
            total = conv_call(lead_parts, 0, None, input_both, bias, cols)
            parts, part_index, edges = lead_parts, 1, lead_edges
            sides = [(lead_edges, 0, input_both)]
        else:
            late = time_index > 1
            total = conv_call(
                rest_parts, time_index - 1, rest_edges if late else None, input_both, bias, cols
            )
            parts, part_index = gathered(hidden), 0
            edges = edges_of(parts)
            sides = [] if late else [(rest_edges, time_index - 1, input_both)]
        sides.append((edges, part_index, hidden_both))
        total = conv_call(parts, part_index, None, hidden_both, total, cols)
        hidden, *cells = gate_call(sides, total, cells, cols, time_index == 0, time_index == steps - 1)

    image = jnp.pad(hidden.reshape(rows, cols, width), ((0, 0), (margin, margin), (0, 0)))

    def columns_for(k):
        piece = lax.dynamic_slice_in_dim(image, starts[k], tile, axis=1, allow_negative_indices=False)
        return piece.reshape(rows * tile, width)

    tiles = [columns_for(0)] + [
        lax.ppermute(columns_for(k), "hid", [(i, i ^ (2 * k)) for i in range(2 * groups)]) for k in range(1, groups)
    ]
    rim = 2 * tile
    tile_edges = swapped_edges(
        jnp.stack([part[:rim] for part in tiles])[None],
        jnp.stack([part[rows * tile - rim :] for part in tiles])[None],
    )
    decoded = decoder_call(
        tiles, tile_edges, first_weight, first_bias, second_weight, second_bias, rows, tile, margin, inner
    )
    decoded = decoded.reshape(rows, tile, -1)
    mine, other = (
        lax.dynamic_slice_in_dim(decoded, start, inner // 2, axis=1, allow_negative_indices=False)
        for start in out_starts
    )
    other = swap(other)
    decoded = jnp.where(core == 0, jnp.stack([mine, other]), jnp.stack([other, mine]))

    cell_mine = cells[0].reshape(rows, cols, share)
    cell_other = swap(cells[1]).reshape(rows, cols, share)
    cell_final = jnp.where(core == 0, jnp.stack([cell_mine, cell_other]), jnp.stack([cell_other, cell_mine]))
    return decoded, cell_final


def solution(mesh):
    return jax.shard_map(
        program,
        mesh=mesh,
        in_specs=(
            P(None, None, "patch", None, "hid"),
            P(None, "patch", None, "hid"),
            P(None, "patch", None, "hid"),
            P(None, None, None, None, "hid"),
            P(None, None, None, None, "hid"),
            P(None, "hid"),
            P(),
            P(),
            P(),
            P(),
        ),
        out_specs=(P(None, "patch", "hid", None), P(None, "patch", None, "hid")),
        check_vma=False,
    )
```

```python
import functools

import jax
import jax.numpy as jnp
from jax import lax
from jax.experimental import pallas as pl
from jax.experimental.pallas import tpu as pltpu
from jax.sharding import PartitionSpec as P


FORGET_BIAS = 1.0
NT = (((1,), (1,)), ((), ()))
NN = (((1,), (0,)), ((), ()))


def place_columns(dst, row0, pieces, group, cols, masked):
    count, width = pieces[0].shape
    groups = len(pieces)
    place = lax.rem(lax.broadcasted_iota(jnp.int32, (count, width), 0), cols)

    def shifts(piece):
        wide = piece.astype(jnp.float32)
        low = pltpu.roll(wide, 1, 0)
        high = pltpu.roll(wide, count - 1, 0)
        if masked:
            low = jnp.where(place == 0, 0.0, low)
            high = jnp.where(place == cols - 1, 0.0, high)
        return (low.astype(dst.dtype), wide.astype(dst.dtype), high.astype(dst.dtype))

    shifted = [shifts(piece) for piece in pieces]
    rows = pl.ds(row0, count)
    if width % 128 == 0:
        for k in range(groups):
            lanes = pl.ds(pl.multiple_of(lax.bitwise_xor(group, k) * width, width), width)
            for q in range(3):
                dst[q, rows, lanes] = shifted[k][q]
    else:
        for j in range(groups):

            @pl.when(group == j)
            def _():
                for q in range(3):
                    dst[q, rows, :] = jnp.concatenate(
                        [shifted[j ^ i][q] for i in range(groups)], axis=1
                    )


def halo_pieces(a_ref, b_ref, index):
    patch = lax.axis_index("patch")
    even = lax.rem(patch, 2) == 0
    above = patch > 0
    below = patch < lax.axis_size("patch") - 1
    top, bottom = [], []
    for k in range(a_ref.shape[1]):
        a = a_ref[index, k].astype(jnp.float32)
        b = b_ref[index, k].astype(jnp.float32)
        top.append(jnp.where(above, jnp.where(even, b, a), 0.0))
        bottom.append(jnp.where(below, jnp.where(even, a, b), 0.0))
    return top, bottom


def stage_kernel(*refs):
    sources, target, semaphores = refs[:-2], refs[-2], refs[-1]
    copies = []
    for p in range(3):
        for q in range(3):
            for i, source in enumerate(sources):
                copy = pltpu.make_async_copy(source.at[p, q], target.at[p, q, i], semaphores.at[p, q, i])
                copy.start()
                copies.append(copy)
    for copy in copies:
        copy.wait()


def tap(weight_ref, p, q):
    weight = weight_ref[p, q]
    return weight.reshape(-1, weight.shape[-1])


def conv_kernel(groups, cols, index, halo, *refs):
    refs = list(refs)
    parts = [refs.pop(0) for _ in range(groups)]
    if halo:
        edge_a, edge_b = refs.pop(0), refs.pop(0)
    weight_ref, init_ref, out_ref, held = refs
    count = out_ref.shape[1]
    group = lax.axis_index("hid") // 2

    place_columns(held, cols, [part[index] for part in parts], group, cols, True)
    if halo:
        top, bottom = halo_pieces(edge_a, edge_b, index)
        place_columns(held, 0, top, group, cols, True)
        place_columns(held, cols + count, bottom, group, cols, True)
    else:
        zero = jnp.zeros((cols, held.shape[2]), held.dtype)
        for q in range(3):
            held[q, pl.ds(0, cols), :] = zero
            held[q, pl.ds(cols + count, cols), :] = zero
    if init_ref.shape == out_ref.shape:
        total = init_ref[...]
    else:
        column = jnp.broadcast_to(init_ref[...], (8, out_ref.shape[0])).T
        total = jnp.broadcast_to(column[:, :1], out_ref.shape)
    for p in range(3):
        for q in range(3):
            window = held[q, p * cols : p * cols + count, :]
            total = total + lax.dot_general(
                tap(weight_ref, p, q), window, NT, preferred_element_type=jnp.float32
            )
    out_ref[...] = total


def gate_kernel(cols, indices, turn_in, turn_out, *refs):
    refs = list(refs)
    sides = [(refs.pop(0), refs.pop(0), refs.pop(0), index) for index in indices]
    total_ref = refs.pop(0)
    cells = [refs.pop(0), refs.pop(0)]
    hidden_ref = refs.pop(0)
    cells_out = [refs.pop(0), refs.pop(0)]
    held, turned, summed = refs
    group = lax.axis_index("hid") // 2
    core = lax.rem(lax.axis_index("hid"), 2)
    count = total_ref.shape[1]
    channels = total_ref.shape[0] // 8
    side = 2 * cols

    summed[...] = total_ref[...]
    zero = jnp.zeros((cols, held.shape[2]), held.dtype)
    for q in range(3):
        held[q, pl.ds(cols, cols), :] = zero
        held[q, pl.ds(2 * cols, cols), :] = zero
    for edge_a, edge_b, weight_ref, index in sides:
        top, bottom = halo_pieces(edge_a, edge_b, index)
        place_columns(held, 0, top, group, cols, True)
        place_columns(held, 3 * cols, bottom, group, cols, True)
        for p, row0, lane0 in ((0, 0, 0), (2, side, count - side)):
            total = summed[:, lane0 : lane0 + side]
            for q in range(3):
                window = held[q, row0 : row0 + side, :]
                total = total + lax.dot_general(
                    tap(weight_ref, p, q), window, NT, preferred_element_type=jnp.float32
                )
            summed[:, lane0 : lane0 + side] = total
    for half in range(2):
        base = half * 4 * channels
        z0, z1, z2, z3 = (summed[base + i * channels : base + (i + 1) * channels, :] for i in range(4))
        cell = cells[half][...].T if turn_in else cells[half][...]
        cell = jax.nn.sigmoid(z1 + FORGET_BIAS) * cell + jax.nn.sigmoid(z0) * jnp.tanh(z2)
        cells_out[half][...] = cell.T if turn_out else cell
        rows = pl.ds(pl.multiple_of(lax.bitwise_xor(core, half) * channels, channels), channels)
        turned[rows, :] = jax.nn.sigmoid(z3) * jnp.tanh(cell)
    hidden_ref[0] = turned[...].T.astype(hidden_ref.dtype)


def decoder_kernel(groups, rows, width, margin, inner, *refs):
    parts = refs[:groups]
    edge_a, edge_b, first_ref, bias1_ref, second_ref, bias2_ref, out_ref, held, middle = refs[groups:]
    group = lax.axis_index("hid") // 2
    patch = lax.axis_index("patch")
    image_rows = rows * lax.axis_size("patch")
    image_cols = inner * groups

    def conv(source, weight_ref, bias_ref, count):
        total = jnp.broadcast_to(bias_ref[...], (count * width, bias_ref.shape[1]))
        for p in range(3):
            for q in range(3):
                window = source[q, p * width : (p + count) * width, :]
                total = total + lax.dot_general(
                    window, tap(weight_ref, p, q), NN, preferred_element_type=jnp.float32
                )
        return total

    top, bottom = halo_pieces(edge_a, edge_b, 0)
    place_columns(held, 0, top, group, width, False)
    place_columns(held, 2 * width, [part[...] for part in parts], group, width, False)
    place_columns(held, (2 + rows) * width, bottom, group, width, False)
    value = conv(held, first_ref, bias1_ref, rows + 2)
    place = lax.broadcasted_iota(jnp.int32, value.shape, 0)
    row = patch * rows + place // width - 1
    col = group * inner - margin + lax.rem(place, width)
    inside = (row >= 0) & (row < image_rows) & (col >= 0) & (col < image_cols)
    value = jnp.where(inside, value * jax.nn.sigmoid(value), 0.0)
    value = value.astype(middle.dtype).astype(jnp.float32)
    middle[0] = pltpu.roll(value, 1, 0).astype(middle.dtype)
    middle[1] = value.astype(middle.dtype)
    middle[2] = pltpu.roll(value, value.shape[0] - 1, 0).astype(middle.dtype)
    out_ref[...] = conv(middle, second_ref, bias2_ref, rows).astype(out_ref.dtype)


WHOLE = pl.BlockSpec(memory_space=pltpu.VMEM)
VMEM_LIMIT = 10 * 1024 * 1024


def params():
    return pltpu.CompilerParams(vmem_limit_bytes=VMEM_LIMIT)


def cost(flops, size):
    return pl.CostEstimate(flops=flops, bytes_accessed=size, transcendentals=0)


def stage_call(*sources):
    shape = sources[0].shape[:2] + (len(sources),) + sources[0].shape[2:]
    size = 2 * sources[0].size * len(sources)
    return pl.pallas_call(
        stage_kernel,
        in_specs=[pl.BlockSpec(memory_space=pltpu.HBM)] * len(sources),
        out_specs=WHOLE,
        out_shape=pltpu.VMEM(shape, sources[0].dtype),
        scratch_shapes=[pltpu.SemaphoreType.DMA((3, 3, len(sources)))],
        compiler_params=params(),
        cost_estimate=cost(100 * size, size),
    )(*(pltpu.with_memory_space_constraint(source, pltpu.HBM) for source in sources))


def conv_call(parts, index, edges, weight, init, cols):
    groups = len(parts)
    count = parts[0].shape[1]
    channels = weight.shape[-1]
    outs = 2 * weight.shape[3]
    operands = list(parts) + ([] if edges is None else list(edges)) + [weight, init]
    return pl.pallas_call(
        functools.partial(conv_kernel, groups, cols, index, edges is not None),
        in_specs=[WHOLE] * len(operands),
        out_specs=WHOLE,
        out_shape=jax.ShapeDtypeStruct((outs, count), jnp.float32),
        scratch_shapes=[pltpu.VMEM((3, count + 2 * cols, channels), jnp.bfloat16)],
        compiler_params=params(),
        cost_estimate=cost(2 * outs * count * 9 * channels, 18 * outs * channels),
    )(*operands)


def gate_call(sides, total, cells, cols, turn_in, turn_out):
    outs, count = total.shape
    channels = sides[0][2].shape[-1]
    share = outs // 8
    width = 2 * share
    cell_shape = (count, share) if turn_out else (share, count)
    operands = []
    for edges, _, weight in sides:
        operands += [*edges, weight]
    operands += [total, *cells]
    return pl.pallas_call(
        functools.partial(gate_kernel, cols, [index for _, index, _ in sides], turn_in, turn_out),
        in_specs=[WHOLE] * len(operands),
        out_specs=[WHOLE] * 3,
        out_shape=[jax.ShapeDtypeStruct((1, count, width), jnp.bfloat16)]
        + [jax.ShapeDtypeStruct(cell_shape, jnp.float32)] * 2,
        scratch_shapes=[
            pltpu.VMEM((3, 4 * cols, channels), jnp.bfloat16),
            pltpu.VMEM((width, count), jnp.float32),
            pltpu.VMEM((outs, count), jnp.float32),
        ],
        compiler_params=params(),
        cost_estimate=cost(2 * outs * count * 6 * channels, 12 * outs * channels),
    )(*operands)


def decoder_call(parts, edges, first, first_bias, second, second_bias, rows, width, margin, inner):
    groups = len(parts)
    channels = first.shape[3]
    outs = second.shape[4]
    operands = [*parts, *edges, first, first_bias.reshape(1, -1), second, second_bias.reshape(1, -1)]
    return pl.pallas_call(
        functools.partial(decoder_kernel, groups, rows, width, margin, inner),
        in_specs=[WHOLE] * len(operands),
        out_specs=WHOLE,
        out_shape=jax.ShapeDtypeStruct((rows * width, outs), jnp.bfloat16),
        scratch_shapes=[
            pltpu.VMEM((3, (rows + 4) * width, channels), jnp.bfloat16),
            pltpu.VMEM((3, (rows + 2) * width, first.shape[4]), jnp.bfloat16),
        ],
        compiler_params=params(),
        cost_estimate=cost(18 * channels * outs * (2 * rows + 2) * width, 36 * channels * outs),
    )(*operands)


def program(
    frames,
    hidden_start,
    cell_start,
    input_weight,
    hidden_weight,
    gate_bias,
    first_weight,
    first_bias,
    second_weight,
    second_bias,
):
    steps, batch, rows, cols, share = frames.shape
    groups = lax.axis_size("hid") // 2
    patches = lax.axis_size("patch")
    assert batch == 2 and groups & (groups - 1) == 0 and patches % 2 == 0
    hid = lax.axis_index("hid")
    core = lax.rem(hid, 2)
    group = hid // 2
    even = lax.rem(lax.axis_index("patch"), 2) == 0
    count = rows * cols
    width = 2 * share

    pairs = [(i, i ^ 1) for i in range(2 * groups)]
    inner_pairs = [(i, i ^ 1) for i in range(patches)]
    outer_pairs = [(i, (i - 1) % patches if i % 2 == 0 else (i + 1) % patches) for i in range(patches)]

    def swap(value):
        return lax.ppermute(value, "hid", pairs)

    def own_batch(value, axis):
        mine = lax.dynamic_index_in_dim(value, core, axis, keepdims=False, allow_negative_indices=False)
        other = lax.dynamic_index_in_dim(value, 1 - core, axis, keepdims=False, allow_negative_indices=False)
        return mine, swap(other)

    def gathered(value):
        return [value] + [
            lax.ppermute(value, "hid", [(i, i ^ (2 * k)) for i in range(2 * groups)]) for k in range(1, groups)
        ]

    def swapped_edges(top, bottom):
        first = lax.ppermute(jnp.where(even, bottom, top), "patch", inner_pairs)
        second = lax.ppermute(jnp.where(even, top, bottom), "patch", outer_pairs)
        return first, second

    def edges_of(parts):
        top = jnp.stack([part[:, :cols] for part in parts], 1)
        bottom = jnp.stack([part[:, count - cols :] for part in parts], 1)
        return swapped_edges(top, bottom)

    def gate_major(weight):
        turned = jnp.transpose(weight, (0, 1, 3, 4, 2))
        return turned.reshape(turned.shape[:2] + (-1,) + turned.shape[-1:])

    def ordered(mine, other, axis):
        return jnp.where(core == 0, jnp.concatenate([mine, other], axis), jnp.concatenate([other, mine], axis))

    def frames_of(index, first):
        size = (steps - 1 if first else 1, 1) + frames.shape[2:]
        return lax.dynamic_slice(frames, (first, index, 0, 0, 0), size, allow_negative_indices=False)[:, 0]

    def of_batch(index):
        state = lax.dynamic_slice_in_dim(hidden_start, index, 1, 0, allow_negative_indices=False)
        return jnp.concatenate([frames_of(index, 0), state], 0)

    lead = ordered(of_batch(core), swap(of_batch(1 - core)), -1).reshape(2, count, width)
    inner = cols // groups
    tile = -(-(inner + 4) // 16) * 16
    margin = (tile - inner) // 2
    starts = [lax.bitwise_xor(group, k) * inner for k in range(groups)]
    out_starts = [margin + core * (inner // 2), margin + (1 - core) * (inner // 2)]
    (lead, starts, out_starts), frames, cell_start, gate_bias, input_own, hidden_own, first_weight, second_weight = (
        lax.optimization_barrier(
            (
                (lead, starts, out_starts),
                frames,
                cell_start,
                gate_bias,
                gate_major(input_weight),
                gate_major(hidden_weight),
                first_weight,
                second_weight,
            )
        )
    )
    lead_parts = gathered(lead)
    input_pair, hidden_pair = swap(input_own), swap(hidden_own)
    input_both = stage_call(input_own, input_pair)
    hidden_both = stage_call(hidden_own, hidden_pair)
    first_weight = stage_call(first_weight)
    second_weight = stage_call(second_weight)
    rest = ordered(frames_of(core, 1), swap(frames_of(1 - core, 1)), -1).reshape(steps - 1, count, width)
    cell_mine, cell_other = own_batch(cell_start, 0)
    cells = [cell_mine.reshape(count, share), cell_other.reshape(count, share)]
    bias_own = gate_bias.reshape(-1)
    bias = jnp.concatenate([bias_own, swap(bias_own)]).reshape(1, -1)

    lead_parts, cells, bias = lax.optimization_barrier((lead_parts, cells, bias))
    lead_edges = edges_of(lead_parts)
    rest_parts = gathered(rest)
    rest_edges = edges_of(rest_parts)

    for time_index in range(steps):
        if time_index == 0:
            total = conv_call(lead_parts, 0, None, input_both, bias, cols)
            parts, part_index, edges = lead_parts, 1, lead_edges
            sides = [(lead_edges, 0, input_both)]
        else:
            late = time_index > 1
            total = conv_call(
                rest_parts, time_index - 1, rest_edges if late else None, input_both, bias, cols
            )
            parts, part_index = gathered(hidden), 0
            edges = edges_of(parts)
            sides = [] if late else [(rest_edges, time_index - 1, input_both)]
        sides.append((edges, part_index, hidden_both))
        total = conv_call(parts, part_index, None, hidden_both, total, cols)
        hidden, *cells = gate_call(sides, total, cells, cols, time_index == 0, time_index == steps - 1)

    image = jnp.pad(hidden.reshape(rows, cols, width), ((0, 0), (margin, margin), (0, 0)))

    def columns_for(k):
        piece = lax.dynamic_slice_in_dim(image, starts[k], tile, axis=1, allow_negative_indices=False)
        return piece.reshape(rows * tile, width)

    tiles = [columns_for(0)] + [
        lax.ppermute(columns_for(k), "hid", [(i, i ^ (2 * k)) for i in range(2 * groups)])
        for k in range(1, groups)
    ]
    rim = 2 * tile
    tile_edges = swapped_edges(
        jnp.stack([part[:rim] for part in tiles])[None],
        jnp.stack([part[rows * tile - rim :] for part in tiles])[None],
    )
    decoded = decoder_call(
        tiles, tile_edges, first_weight, first_bias, second_weight, second_bias, rows, tile, margin, inner
    )
    decoded = decoded.reshape(rows, tile, -1)
    mine, other = (
        lax.dynamic_slice_in_dim(decoded, start, inner // 2, axis=1, allow_negative_indices=False)
        for start in out_starts
    )
    other = swap(other)
    decoded = jnp.where(core == 0, jnp.stack([mine, other]), jnp.stack([other, mine]))

    cell_mine = cells[0].reshape(rows, cols, share)
    cell_other = swap(cells[1]).reshape(rows, cols, share)
    cell_final = jnp.where(core == 0, jnp.stack([cell_mine, cell_other]), jnp.stack([cell_other, cell_mine]))
    return decoded, cell_final


def solution(mesh):
    return jax.shard_map(
        program,
        mesh=mesh,
        in_specs=(
            P(None, None, "patch", None, "hid"),
            P(None, "patch", None, "hid"),
            P(None, "patch", None, "hid"),
            P(None, None, None, None, "hid"),
            P(None, None, None, None, "hid"),
            P(None, "hid"),
            P(),
            P(),
            P(),
            P(),
        ),
        out_specs=(P(None, "patch", "hid", None), P(None, "patch", None, "hid")),
        check_vma=False,
    )
```

```python
import functools

import jax
import jax.numpy as jnp
from jax import lax
from jax.experimental import pallas as pl
from jax.experimental.pallas import tpu as pltpu
from jax.sharding import PartitionSpec as P


FORGET_BIAS = 1.0
NT = (((1,), (1,)), ((), ()))
NN = (((1,), (0,)), ((), ()))


def place_columns(dst, row0, pieces, group, cols, masked):
    count, width = pieces[0].shape
    groups = len(pieces)
    place = lax.rem(lax.broadcasted_iota(jnp.int32, (count, width), 0), cols)

    def shifts(piece):
        wide = piece.astype(jnp.float32)
        low = pltpu.roll(wide, 1, 0)
        high = pltpu.roll(wide, count - 1, 0)
        if masked:
            low = jnp.where(place == 0, 0.0, low)
            high = jnp.where(place == cols - 1, 0.0, high)
        return (low.astype(dst.dtype), wide.astype(dst.dtype), high.astype(dst.dtype))

    shifted = [shifts(piece) for piece in pieces]
    rows = pl.ds(row0, count)
    if width % 128 == 0:
        for k in range(groups):
            lanes = pl.ds(pl.multiple_of(lax.bitwise_xor(group, k) * width, width), width)
            for q in range(3):
                dst[q, rows, lanes] = shifted[k][q]
    else:
        for j in range(groups):

            @pl.when(group == j)
            def _():
                for q in range(3):
                    dst[q, rows, :] = jnp.concatenate(
                        [shifted[j ^ i][q] for i in range(groups)], axis=1
                    )


def halo_pieces(a_ref, b_ref, index):
    patch = lax.axis_index("patch")
    even = lax.rem(patch, 2) == 0
    above = patch > 0
    below = patch < lax.axis_size("patch") - 1
    top, bottom = [], []
    for k in range(a_ref.shape[1]):
        a = a_ref[index, k].astype(jnp.float32)
        b = b_ref[index, k].astype(jnp.float32)
        top.append(jnp.where(above, jnp.where(even, b, a), 0.0))
        bottom.append(jnp.where(below, jnp.where(even, a, b), 0.0))
    return top, bottom


def stage_kernel(*refs):
    sources, target, semaphores = refs[:-2], refs[-2], refs[-1]
    copies = []
    for p in range(3):
        for q in range(3):
            for i, source in enumerate(sources):
                copy = pltpu.make_async_copy(source.at[p, q], target.at[p, q, i], semaphores.at[p, q, i])
                copy.start()
                copies.append(copy)
    for copy in copies:
        copy.wait()


def tap(weight_ref, p, q):
    weight = weight_ref[p, q]
    return weight.reshape(-1, weight.shape[-1])


def conv_kernel(groups, cols, index, halo, *refs):
    refs = list(refs)
    parts = [refs.pop(0) for _ in range(groups)]
    if halo:
        edge_a, edge_b = refs.pop(0), refs.pop(0)
    weight_ref, init_ref, out_ref, held = refs
    count = out_ref.shape[1]
    group = lax.axis_index("hid") // 2

    place_columns(held, cols, [part[index] for part in parts], group, cols, True)
    if halo:
        top, bottom = halo_pieces(edge_a, edge_b, index)
        place_columns(held, 0, top, group, cols, True)
        place_columns(held, cols + count, bottom, group, cols, True)
    else:
        zero = jnp.zeros((cols, held.shape[2]), held.dtype)
        for q in range(3):
            held[q, pl.ds(0, cols), :] = zero
            held[q, pl.ds(cols + count, cols), :] = zero
    if init_ref.shape == out_ref.shape:
        total = init_ref[...]
    else:
        column = jnp.broadcast_to(init_ref[...], (8, out_ref.shape[0])).T
        total = jnp.broadcast_to(column[:, :1], out_ref.shape)
    for p in range(3):
        for q in range(3):
            window = held[q, p * cols : p * cols + count, :]
            total = total + lax.dot_general(
                tap(weight_ref, p, q), window, NT, preferred_element_type=jnp.float32
            )
    out_ref[...] = total


def gate_kernel(cols, indices, turn_in, turn_out, *refs):
    refs = list(refs)
    sides = [(refs.pop(0), refs.pop(0), refs.pop(0), index) for index in indices]
    total_ref = refs.pop(0)
    cells = [refs.pop(0), refs.pop(0)]
    hidden_ref = refs.pop(0)
    cells_out = [refs.pop(0), refs.pop(0)]
    held, turned, summed = refs
    group = lax.axis_index("hid") // 2
    core = lax.rem(lax.axis_index("hid"), 2)
    count = total_ref.shape[1]
    channels = total_ref.shape[0] // 8
    side = 2 * cols

    summed[...] = total_ref[...]
    zero = jnp.zeros((cols, held.shape[2]), held.dtype)
    for q in range(3):
        held[q, pl.ds(cols, cols), :] = zero
        held[q, pl.ds(2 * cols, cols), :] = zero
    for edge_a, edge_b, weight_ref, index in sides:
        top, bottom = halo_pieces(edge_a, edge_b, index)
        place_columns(held, 0, top, group, cols, True)
        place_columns(held, 3 * cols, bottom, group, cols, True)
        for p, row0, lane0 in ((0, 0, 0), (2, side, count - side)):
            total = summed[:, lane0 : lane0 + side]
            for q in range(3):
                window = held[q, row0 : row0 + side, :]
                total = total + lax.dot_general(
                    tap(weight_ref, p, q), window, NT, preferred_element_type=jnp.float32
                )
            summed[:, lane0 : lane0 + side] = total
    for half in range(2):
        base = half * 4 * channels
        z0, z1, z2, z3 = (summed[base + i * channels : base + (i + 1) * channels, :] for i in range(4))
        cell = cells[half][...].T if turn_in else cells[half][...]
        cell = jax.nn.sigmoid(z1 + FORGET_BIAS) * cell + jax.nn.sigmoid(z0) * jnp.tanh(z2)
        cells_out[half][...] = cell.T if turn_out else cell
        rows = pl.ds(pl.multiple_of(lax.bitwise_xor(core, half) * channels, channels), channels)
        turned[rows, :] = jax.nn.sigmoid(z3) * jnp.tanh(cell)
    hidden_ref[0] = turned[...].T.astype(hidden_ref.dtype)


def decoder_kernel(groups, rows, width, margin, inner, *refs):
    parts = refs[:groups]
    edge_a, edge_b, first_ref, bias1_ref, second_ref, bias2_ref, out_ref, held, middle = refs[groups:]
    group = lax.axis_index("hid") // 2
    patch = lax.axis_index("patch")
    image_rows = rows * lax.axis_size("patch")
    image_cols = inner * groups

    def conv(source, weight_ref, bias_ref, count):
        total = jnp.broadcast_to(bias_ref[...], (count * width, bias_ref.shape[1]))
        for p in range(3):
            for q in range(3):
                window = source[q, p * width : (p + count) * width, :]
                total = total + lax.dot_general(
                    window, tap(weight_ref, p, q), NN, preferred_element_type=jnp.float32
                )
        return total

    top, bottom = halo_pieces(edge_a, edge_b, 0)
    place_columns(held, 0, top, group, width, False)
    place_columns(held, 2 * width, [part[...] for part in parts], group, width, False)
    place_columns(held, (2 + rows) * width, bottom, group, width, False)
    value = conv(held, first_ref, bias1_ref, rows + 2)
    place = lax.broadcasted_iota(jnp.int32, value.shape, 0)
    row = patch * rows + place // width - 1
    col = group * inner - margin + lax.rem(place, width)
    inside = (row >= 0) & (row < image_rows) & (col >= 0) & (col < image_cols)
    value = jnp.where(inside, value * jax.nn.sigmoid(value), 0.0)
    value = value.astype(middle.dtype).astype(jnp.float32)
    middle[0] = pltpu.roll(value, 1, 0).astype(middle.dtype)
    middle[1] = value.astype(middle.dtype)
    middle[2] = pltpu.roll(value, value.shape[0] - 1, 0).astype(middle.dtype)
    out_ref[...] = conv(middle, second_ref, bias2_ref, rows).astype(out_ref.dtype)


WHOLE = pl.BlockSpec(memory_space=pltpu.VMEM)
VMEM_LIMIT = 10 * 1024 * 1024


def params():
    return pltpu.CompilerParams(vmem_limit_bytes=VMEM_LIMIT)


def cost(flops, size):
    return pl.CostEstimate(flops=flops, bytes_accessed=size, transcendentals=0)


def stage_call(*sources):
    shape = sources[0].shape[:2] + (len(sources),) + sources[0].shape[2:]
    size = 2 * sources[0].size * len(sources)
    return pl.pallas_call(
        stage_kernel,
        in_specs=[pl.BlockSpec(memory_space=pltpu.HBM)] * len(sources),
        out_specs=WHOLE,
        out_shape=pltpu.VMEM(shape, sources[0].dtype),
        scratch_shapes=[pltpu.SemaphoreType.DMA((3, 3, len(sources)))],
        compiler_params=params(),
        cost_estimate=cost(100 * size, size),
    )(*(pltpu.with_memory_space_constraint(source, pltpu.HBM) for source in sources))


def conv_call(parts, index, edges, weight, init, cols):
    groups = len(parts)
    count = parts[0].shape[1]
    channels = weight.shape[-1]
    outs = 2 * weight.shape[3]
    operands = list(parts) + ([] if edges is None else list(edges)) + [weight, init]
    return pl.pallas_call(
        functools.partial(conv_kernel, groups, cols, index, edges is not None),
        in_specs=[WHOLE] * len(operands),
        out_specs=WHOLE,
        out_shape=jax.ShapeDtypeStruct((outs, count), jnp.float32),
        scratch_shapes=[pltpu.VMEM((3, count + 2 * cols, channels), jnp.bfloat16)],
        compiler_params=params(),
        cost_estimate=cost(2 * outs * count * 9 * channels, 18 * outs * channels),
    )(*operands)


def gate_call(sides, total, cells, cols, turn_in, turn_out):
    outs, count = total.shape
    channels = sides[0][2].shape[-1]
    share = outs // 8
    width = 2 * share
    cell_shape = (count, share) if turn_out else (share, count)
    operands = []
    for edges, _, weight in sides:
        operands += [*edges, weight]
    operands += [total, *cells]
    return pl.pallas_call(
        functools.partial(gate_kernel, cols, [index for _, index, _ in sides], turn_in, turn_out),
        in_specs=[WHOLE] * len(operands),
        out_specs=[WHOLE] * 3,
        out_shape=[jax.ShapeDtypeStruct((1, count, width), jnp.bfloat16)]
        + [jax.ShapeDtypeStruct(cell_shape, jnp.float32)] * 2,
        scratch_shapes=[
            pltpu.VMEM((3, 4 * cols, channels), jnp.bfloat16),
            pltpu.VMEM((width, count), jnp.float32),
            pltpu.VMEM((outs, count), jnp.float32),
        ],
        compiler_params=params(),
        cost_estimate=cost(2 * outs * count * 6 * channels, 12 * outs * channels),
    )(*operands)


def decoder_call(parts, edges, first, first_bias, second, second_bias, rows, width, margin, inner):
    groups = len(parts)
    channels = first.shape[3]
    outs = second.shape[4]
    operands = [*parts, *edges, first, first_bias.reshape(1, -1), second, second_bias.reshape(1, -1)]
    return pl.pallas_call(
        functools.partial(decoder_kernel, groups, rows, width, margin, inner),
        in_specs=[WHOLE] * len(operands),
        out_specs=WHOLE,
        out_shape=jax.ShapeDtypeStruct((rows * width, outs), jnp.bfloat16),
        scratch_shapes=[
            pltpu.VMEM((3, (rows + 4) * width, channels), jnp.bfloat16),
            pltpu.VMEM((3, (rows + 2) * width, first.shape[4]), jnp.bfloat16),
        ],
        compiler_params=params(),
        cost_estimate=cost(18 * channels * outs * (2 * rows + 2) * width, 36 * channels * outs),
    )(*operands)


def program(
    frames,
    hidden_start,
    cell_start,
    input_weight,
    hidden_weight,
    gate_bias,
    first_weight,
    first_bias,
    second_weight,
    second_bias,
):
    steps, batch, rows, cols, share = frames.shape
    groups = lax.axis_size("hid") // 2
    patches = lax.axis_size("patch")
    assert batch == 2 and groups & (groups - 1) == 0 and patches % 2 == 0
    hid = lax.axis_index("hid")
    core = lax.rem(hid, 2)
    group = hid // 2
    even = lax.rem(lax.axis_index("patch"), 2) == 0
    count = rows * cols
    width = 2 * share

    pairs = [(i, i ^ 1) for i in range(2 * groups)]
    inner_pairs = [(i, i ^ 1) for i in range(patches)]
    outer_pairs = [(i, (i - 1) % patches if i % 2 == 0 else (i + 1) % patches) for i in range(patches)]

    def swap(value):
        return lax.ppermute(value, "hid", pairs)

    def own_batch(value, axis):
        mine = lax.dynamic_index_in_dim(value, core, axis, keepdims=False, allow_negative_indices=False)
        other = lax.dynamic_index_in_dim(value, 1 - core, axis, keepdims=False, allow_negative_indices=False)
        return mine, swap(other)

    def gathered(value):
        return [value] + [
            lax.ppermute(value, "hid", [(i, i ^ (2 * k)) for i in range(2 * groups)]) for k in range(1, groups)
        ]

    def across(value, k):
        return lax.ppermute(value, "hid", [(i, i ^ (2 * k)) for i in range(2 * groups)])

    def forwarded(value):
        parts = [value]
        parts += [across(value, k) for k in range(1, groups) if k == 1 or k % 2 == 0]
        near = dict(zip([0, 1] + [k for k in range(2, groups, 2)], parts))
        for k in range(3, groups, 2):
            near[k] = across(near[k - 1], 1)
        return [near[k] for k in range(groups)]

    def swapped_edges(top, bottom):
        first = lax.ppermute(jnp.where(even, bottom, top), "patch", inner_pairs)
        second = lax.ppermute(jnp.where(even, top, bottom), "patch", outer_pairs)
        return first, second

    def edges_of(parts):
        top = jnp.stack([part[:, :cols] for part in parts], 1)
        bottom = jnp.stack([part[:, count - cols :] for part in parts], 1)
        return swapped_edges(top, bottom)

    def gate_major(weight):
        turned = jnp.transpose(weight, (0, 1, 3, 4, 2))
        return turned.reshape(turned.shape[:2] + (-1,) + turned.shape[-1:])

    def ordered(mine, other, axis):
        return jnp.where(core == 0, jnp.concatenate([mine, other], axis), jnp.concatenate([other, mine], axis))

    def frames_of(index, first):
        size = (steps - 1 if first else 1, 1) + frames.shape[2:]
        return lax.dynamic_slice(frames, (first, index, 0, 0, 0), size, allow_negative_indices=False)[:, 0]

    def of_batch(index):
        state = lax.dynamic_slice_in_dim(hidden_start, index, 1, 0, allow_negative_indices=False)
        return jnp.concatenate([frames_of(index, 0), state], 0)

    lead = ordered(of_batch(core), swap(of_batch(1 - core)), -1).reshape(2, count, width)
    inner = cols // groups
    tile = -(-(inner + 4) // 16) * 16
    margin = (tile - inner) // 2
    starts = [lax.bitwise_xor(group, k) * inner for k in range(groups)]
    out_starts = [margin + core * (inner // 2), margin + (1 - core) * (inner // 2)]
    (lead, starts, out_starts), frames, cell_start, gate_bias, input_own, hidden_own, first_weight, second_weight = (
        lax.optimization_barrier(
            (
                (lead, starts, out_starts),
                frames,
                cell_start,
                gate_bias,
                gate_major(input_weight),
                gate_major(hidden_weight),
                first_weight,
                second_weight,
            )
        )
    )
    lead_parts = gathered(lead)
    input_pair, hidden_pair = swap(input_own), swap(hidden_own)
    input_both = stage_call(input_own, input_pair)
    hidden_both = stage_call(hidden_own, hidden_pair)
    first_weight = stage_call(first_weight)
    second_weight = stage_call(second_weight)
    rest = ordered(frames_of(core, 1), swap(frames_of(1 - core, 1)), -1).reshape(steps - 1, count, width)
    cell_mine, cell_other = own_batch(cell_start, 0)
    cells = [cell_mine.reshape(count, share), cell_other.reshape(count, share)]
    bias_own = gate_bias.reshape(-1)
    bias = jnp.concatenate([bias_own, swap(bias_own)]).reshape(1, -1)

    lead_parts, cells, bias = lax.optimization_barrier((lead_parts, cells, bias))
    lead_edges = edges_of(lead_parts)
    rest_parts = forwarded(rest)
    rest_edges = edges_of(rest_parts)

    for time_index in range(steps):
        if time_index == 0:
            total = conv_call(lead_parts, 0, None, input_both, bias, cols)
            parts, part_index, edges = lead_parts, 1, lead_edges
            sides = [(lead_edges, 0, input_both)]
        else:
            late = time_index > 1
            total = conv_call(
                rest_parts, time_index - 1, rest_edges if late else None, input_both, bias, cols
            )
            parts, part_index = gathered(hidden), 0
            edges = edges_of(parts)
            sides = [] if late else [(rest_edges, time_index - 1, input_both)]
        sides.append((edges, part_index, hidden_both))
        total = conv_call(parts, part_index, None, hidden_both, total, cols)
        hidden, *cells = gate_call(sides, total, cells, cols, time_index == 0, time_index == steps - 1)

    image = jnp.pad(hidden.reshape(rows, cols, width), ((0, 0), (margin, margin), (0, 0)))

    def columns_for(k):
        piece = lax.dynamic_slice_in_dim(image, starts[k], tile, axis=1, allow_negative_indices=False)
        return piece.reshape(rows * tile, width)

    tiles = [columns_for(0)] + [
        lax.ppermute(columns_for(k), "hid", [(i, i ^ (2 * k)) for i in range(2 * groups)])
        for k in range(1, groups)
    ]
    rim = 2 * tile
    tile_edges = swapped_edges(
        jnp.stack([part[:rim] for part in tiles])[None],
        jnp.stack([part[rows * tile - rim :] for part in tiles])[None],
    )
    decoded = decoder_call(
        tiles, tile_edges, first_weight, first_bias, second_weight, second_bias, rows, tile, margin, inner
    )
    decoded = decoded.reshape(rows, tile, -1)
    mine, other = (
        lax.dynamic_slice_in_dim(decoded, start, inner // 2, axis=1, allow_negative_indices=False)
        for start in out_starts
    )
    other = swap(other)
    decoded = jnp.where(core == 0, jnp.stack([mine, other]), jnp.stack([other, mine]))

    cell_mine = cells[0].reshape(rows, cols, share)
    cell_other = swap(cells[1]).reshape(rows, cols, share)
    cell_final = jnp.where(core == 0, jnp.stack([cell_mine, cell_other]), jnp.stack([cell_other, cell_mine]))
    return decoded, cell_final


def solution(mesh):
    return jax.shard_map(
        program,
        mesh=mesh,
        in_specs=(
            P(None, None, "patch", None, "hid"),
            P(None, "patch", None, "hid"),
            P(None, "patch", None, "hid"),
            P(None, None, None, None, "hid"),
            P(None, None, None, None, "hid"),
            P(None, "hid"),
            P(),
            P(),
            P(),
            P(),
        ),
        out_specs=(P(None, "patch", "hid", None), P(None, "patch", None, "hid")),
        check_vma=False,
    )
```

```python
import functools

import jax
import jax.numpy as jnp
from jax import lax
from jax.experimental import pallas as pl
from jax.experimental.pallas import tpu as pltpu
from jax.sharding import PartitionSpec as P


FORGET_BIAS = 1.0
NT = (((1,), (1,)), ((), ()))
NN = (((1,), (0,)), ((), ()))


def place_columns(dst, row0, pieces, group, cols, masked):
    count, width = pieces[0].shape
    groups = len(pieces)
    place = lax.rem(lax.broadcasted_iota(jnp.int32, (count, width), 0), cols)

    def shifts(piece):
        wide = piece.astype(jnp.float32)
        low = pltpu.roll(wide, 1, 0)
        high = pltpu.roll(wide, count - 1, 0)
        if masked:
            low = jnp.where(place == 0, 0.0, low)
            high = jnp.where(place == cols - 1, 0.0, high)
        return (low.astype(dst.dtype), wide.astype(dst.dtype), high.astype(dst.dtype))

    shifted = [shifts(piece) for piece in pieces]
    rows = pl.ds(row0, count)
    if width % 128 == 0:
        for k in range(groups):
            lanes = pl.ds(pl.multiple_of(lax.bitwise_xor(group, k) * width, width), width)
            for q in range(3):
                dst[q, rows, lanes] = shifted[k][q]
    else:
        for j in range(groups):

            @pl.when(group == j)
            def _():
                for q in range(3):
                    dst[q, rows, :] = jnp.concatenate(
                        [shifted[j ^ i][q] for i in range(groups)], axis=1
                    )


def halo_pieces(a_ref, b_ref, index):
    patch = lax.axis_index("patch")
    even = lax.rem(patch, 2) == 0
    above = patch > 0
    below = patch < lax.axis_size("patch") - 1
    top, bottom = [], []
    for k in range(a_ref.shape[0]):
        a = a_ref[k, index].astype(jnp.float32)
        b = b_ref[k, index].astype(jnp.float32)
        top.append(jnp.where(above, jnp.where(even, b, a), 0.0))
        bottom.append(jnp.where(below, jnp.where(even, a, b), 0.0))
    return top, bottom


def stage_kernel(*refs):
    sources, target, semaphores = refs[:-2], refs[-2], refs[-1]
    copies = []
    for p in range(3):
        for q in range(3):
            for i, source in enumerate(sources):
                copy = pltpu.make_async_copy(source.at[p, q], target.at[p, q, i], semaphores.at[p, q, i])
                copy.start()
                copies.append(copy)
    for copy in copies:
        copy.wait()


def tap(weight_refs, p, q):
    weights = [weight_ref[p, q] for weight_ref in weight_refs]
    weights = [weight.reshape(-1, weight.shape[-1]) for weight in weights]
    return weights[0] if len(weights) == 1 else jnp.concatenate(weights, axis=0)


def conv_kernel(groups, cols, index, edge_index, *refs):
    refs = list(refs)
    halo = edge_index is not None
    parts = [refs.pop(0) for _ in range(groups)]
    if halo:
        edge_a, edge_b = refs.pop(0), refs.pop(0)
    *weight_refs, init_ref, out_ref, held = refs
    count = out_ref.shape[1]
    group = lax.axis_index("hid") // 2

    place_columns(held, cols, [part[index] for part in parts], group, cols, True)
    if halo:
        top, bottom = halo_pieces(edge_a, edge_b, edge_index)
        place_columns(held, 0, top, group, cols, True)
        place_columns(held, cols + count, bottom, group, cols, True)
    else:
        zero = jnp.zeros((cols, held.shape[2]), held.dtype)
        for q in range(3):
            held[q, pl.ds(0, cols), :] = zero
            held[q, pl.ds(cols + count, cols), :] = zero
    if init_ref.shape == out_ref.shape:
        total = init_ref[...]
    else:
        column = jnp.broadcast_to(init_ref[...], (8, out_ref.shape[0])).T
        total = jnp.broadcast_to(column[:, :1], out_ref.shape)
    for p in range(3):
        for q in range(3):
            window = held[q, p * cols : p * cols + count, :]
            total = total + lax.dot_general(
                tap(weight_refs, p, q), window, NT, preferred_element_type=jnp.float32
            )
    out_ref[...] = total


def gate_kernel(cols, indices, turn_in, turn_out, *refs):
    refs = list(refs)
    sides = []
    for index, pieces in indices:
        sides.append((refs.pop(0), refs.pop(0), [refs.pop(0) for _ in range(pieces)], index))
    total_ref = refs.pop(0)
    cells = [refs.pop(0), refs.pop(0)]
    hidden_ref = refs.pop(0)
    cells_out = [refs.pop(0), refs.pop(0)]
    held, turned, summed = refs
    group = lax.axis_index("hid") // 2
    core = lax.rem(lax.axis_index("hid"), 2)
    count = total_ref.shape[1]
    channels = total_ref.shape[0] // 8
    side = 2 * cols

    summed[...] = total_ref[...]
    zero = jnp.zeros((cols, held.shape[2]), held.dtype)
    for q in range(3):
        held[q, pl.ds(cols, cols), :] = zero
        held[q, pl.ds(2 * cols, cols), :] = zero
    for edge_a, edge_b, weight_refs, index in sides:
        top, bottom = halo_pieces(edge_a, edge_b, index)
        place_columns(held, 0, top, group, cols, True)
        place_columns(held, 3 * cols, bottom, group, cols, True)
        for p, row0, lane0 in ((0, 0, 0), (2, side, count - side)):
            total = summed[:, lane0 : lane0 + side]
            for q in range(3):
                window = held[q, row0 : row0 + side, :]
                total = total + lax.dot_general(
                    tap(weight_refs, p, q), window, NT, preferred_element_type=jnp.float32
                )
            summed[:, lane0 : lane0 + side] = total
    for half in range(2):
        base = half * 4 * channels
        z0, z1, z2, z3 = (summed[base + i * channels : base + (i + 1) * channels, :] for i in range(4))
        cell = cells[half][...].T if turn_in else cells[half][...]
        cell = jax.nn.sigmoid(z1 + FORGET_BIAS) * cell + jax.nn.sigmoid(z0) * jnp.tanh(z2)
        cells_out[half][...] = cell.T if turn_out else cell
        rows = pl.ds(pl.multiple_of(lax.bitwise_xor(core, half) * channels, channels), channels)
        turned[rows, :] = jax.nn.sigmoid(z3) * jnp.tanh(cell)
    hidden_ref[0] = turned[...].T.astype(hidden_ref.dtype)


def decoder_kernel(groups, rows, width, margin, inner, *refs):
    parts = refs[:groups]
    edge_a, edge_b, first_ref, bias1_ref, second_ref, bias2_ref, out_ref, held, middle = refs[groups:]
    group = lax.axis_index("hid") // 2
    patch = lax.axis_index("patch")
    image_rows = rows * lax.axis_size("patch")
    image_cols = inner * groups

    def conv(source, weight_ref, bias_ref, count):
        total = jnp.broadcast_to(bias_ref[...], (count * width, bias_ref.shape[1]))
        for p in range(3):
            for q in range(3):
                window = source[q, p * width : (p + count) * width, :]
                total = total + lax.dot_general(
                    window, tap([weight_ref], p, q), NN, preferred_element_type=jnp.float32
                )
        return total

    top, bottom = halo_pieces(edge_a, edge_b, 0)
    place_columns(held, 0, top, group, width, False)
    place_columns(held, 2 * width, [part[...] for part in parts], group, width, False)
    place_columns(held, (2 + rows) * width, bottom, group, width, False)
    value = conv(held, first_ref, bias1_ref, rows + 2)
    place = lax.broadcasted_iota(jnp.int32, value.shape, 0)
    row = patch * rows + place // width - 1
    col = group * inner - margin + lax.rem(place, width)
    inside = (row >= 0) & (row < image_rows) & (col >= 0) & (col < image_cols)
    value = jnp.where(inside, value * jax.nn.sigmoid(value), 0.0)
    value = value.astype(middle.dtype).astype(jnp.float32)
    middle[0] = pltpu.roll(value, 1, 0).astype(middle.dtype)
    middle[1] = value.astype(middle.dtype)
    middle[2] = pltpu.roll(value, value.shape[0] - 1, 0).astype(middle.dtype)
    out_ref[...] = conv(middle, second_ref, bias2_ref, rows).astype(out_ref.dtype)


WHOLE = pl.BlockSpec(memory_space=pltpu.VMEM)
VMEM_LIMIT = 10 * 1024 * 1024


def params():
    return pltpu.CompilerParams(vmem_limit_bytes=VMEM_LIMIT)


def cost(flops, size):
    return pl.CostEstimate(flops=flops, bytes_accessed=size, transcendentals=0)


def stage_call(*sources):
    shape = sources[0].shape[:2] + (len(sources),) + sources[0].shape[2:]
    size = 2 * sources[0].size * len(sources)
    return pl.pallas_call(
        stage_kernel,
        in_specs=[pl.BlockSpec(memory_space=pltpu.HBM)] * len(sources),
        out_specs=WHOLE,
        out_shape=pltpu.VMEM(shape, sources[0].dtype),
        scratch_shapes=[pltpu.SemaphoreType.DMA((3, 3, len(sources)))],
        compiler_params=params(),
        cost_estimate=cost(100 * size, size),
    )(*(pltpu.with_memory_space_constraint(source, pltpu.HBM) for source in sources))


def conv_call(parts, index, edges, edge_index, weights, init, cols):
    groups = len(parts)
    count = parts[0].shape[1]
    channels = weights[0].shape[-1]
    outs = 2 * weights[0].shape[3]
    operands = [*parts, *edges, *weights, init]
    return pl.pallas_call(
        functools.partial(conv_kernel, groups, cols, index, edge_index if edges else None),
        in_specs=[WHOLE] * len(operands),
        out_specs=WHOLE,
        out_shape=jax.ShapeDtypeStruct((outs, count), jnp.float32),
        scratch_shapes=[pltpu.VMEM((3, count + 2 * cols, channels), jnp.bfloat16)],
        compiler_params=params(),
        cost_estimate=cost(2 * outs * count * 9 * channels, 18 * outs * channels),
    )(*operands)


def gate_call(sides, total, cells, cols, turn_in, turn_out):
    outs, count = total.shape
    channels = sides[0][2][0].shape[-1]
    share = outs // 8
    width = 2 * share
    cell_shape = (count, share) if turn_out else (share, count)
    operands = []
    for edges, _, weights in sides:
        operands += [*edges, *weights]
    operands += [total, *cells]
    return pl.pallas_call(
        functools.partial(gate_kernel, cols, [(index, len(weights)) for _, index, weights in sides], turn_in, turn_out),
        in_specs=[WHOLE] * len(operands),
        out_specs=[WHOLE] * 3,
        out_shape=[jax.ShapeDtypeStruct((1, count, width), jnp.bfloat16)]
        + [jax.ShapeDtypeStruct(cell_shape, jnp.float32)] * 2,
        scratch_shapes=[
            pltpu.VMEM((3, 4 * cols, channels), jnp.bfloat16),
            pltpu.VMEM((width, count), jnp.float32),
            pltpu.VMEM((outs, count), jnp.float32),
        ],
        compiler_params=params(),
        cost_estimate=cost(2 * outs * count * 6 * channels, 12 * outs * channels),
    )(*operands)


def decoder_call(parts, edges, first, first_bias, second, second_bias, rows, width, margin, inner):
    groups = len(parts)
    channels = first.shape[3]
    outs = second.shape[4]
    operands = [*parts, *edges, first, first_bias.reshape(1, -1), second, second_bias.reshape(1, -1)]
    return pl.pallas_call(
        functools.partial(decoder_kernel, groups, rows, width, margin, inner),
        in_specs=[WHOLE] * len(operands),
        out_specs=WHOLE,
        out_shape=jax.ShapeDtypeStruct((rows * width, outs), jnp.bfloat16),
        scratch_shapes=[
            pltpu.VMEM((3, (rows + 4) * width, channels), jnp.bfloat16),
            pltpu.VMEM((3, (rows + 2) * width, first.shape[4]), jnp.bfloat16),
        ],
        compiler_params=params(),
        cost_estimate=cost(18 * channels * outs * (2 * rows + 2) * width, 36 * channels * outs),
    )(*operands)


def program(
    frames,
    hidden_start,
    cell_start,
    input_weight,
    hidden_weight,
    gate_bias,
    first_weight,
    first_bias,
    second_weight,
    second_bias,
):
    steps, batch, rows, cols, share = frames.shape
    groups = lax.axis_size("hid") // 2
    patches = lax.axis_size("patch")
    assert batch == 2 and groups & (groups - 1) == 0 and patches % 2 == 0
    hid = lax.axis_index("hid")
    core = lax.rem(hid, 2)
    group = hid // 2
    even = lax.rem(lax.axis_index("patch"), 2) == 0
    count = rows * cols
    width = 2 * share

    pairs = [(i, i ^ 1) for i in range(2 * groups)]
    inner_pairs = [(i, i ^ 1) for i in range(patches)]
    outer_pairs = [(i, (i - 1) % patches if i % 2 == 0 else (i + 1) % patches) for i in range(patches)]

    def swap(value):
        return lax.ppermute(value, "hid", pairs)

    def own_batch(value, axis):
        mine = lax.dynamic_index_in_dim(value, core, axis, keepdims=False, allow_negative_indices=False)
        other = lax.dynamic_index_in_dim(value, 1 - core, axis, keepdims=False, allow_negative_indices=False)
        return mine, swap(other)

    def gathered(value):
        return [value] + [
            lax.ppermute(value, "hid", [(i, i ^ (2 * k)) for i in range(2 * groups)]) for k in range(1, groups)
        ]

    def across(value, k):
        return lax.ppermute(value, "hid", [(i, i ^ (2 * k)) for i in range(2 * groups)])

    def forwarded(value):
        parts = [value]
        parts += [across(value, k) for k in range(1, groups) if k == 1 or k % 2 == 0]
        near = dict(zip([0, 1] + [k for k in range(2, groups, 2)], parts))
        for k in range(3, groups, 2):
            near[k] = across(near[k - 1], 1)
        return [near[k] for k in range(groups)]

    def swapped_edges(top, bottom):
        first = lax.ppermute(jnp.where(even, bottom, top), "patch", inner_pairs)
        second = lax.ppermute(jnp.where(even, top, bottom), "patch", outer_pairs)
        return first, second

    def edges_of(parts):
        top = jnp.stack([part[:, :cols] for part in parts])
        bottom = jnp.stack([part[:, count - cols :] for part in parts])
        return swapped_edges(top, bottom)

    def gate_major(weight):
        turned = jnp.transpose(weight, (0, 1, 3, 4, 2))
        return turned.reshape(turned.shape[:2] + (-1,) + turned.shape[-1:])

    def ordered(mine, other, axis):
        return jnp.where(core == 0, jnp.concatenate([mine, other], axis), jnp.concatenate([other, mine], axis))

    def frames_of(index, first):
        size = (steps - 1 if first else 1, 1) + frames.shape[2:]
        return lax.dynamic_slice(frames, (first, index, 0, 0, 0), size, allow_negative_indices=False)[:, 0]

    def of_batch(index):
        state = lax.dynamic_slice_in_dim(hidden_start, index, 1, 0, allow_negative_indices=False)
        return jnp.concatenate([frames_of(index, 0), state], 0)

    lead = ordered(of_batch(core), swap(of_batch(1 - core)), -1).reshape(2, count, width)
    inner = cols // groups
    tile = -(-(inner + 4) // 16) * 16
    margin = (tile - inner) // 2
    starts = [lax.bitwise_xor(group, k) * inner for k in range(groups)]
    out_starts = [margin + core * (inner // 2), margin + (1 - core) * (inner // 2)]
    input_own, hidden_own = gate_major(input_weight), gate_major(hidden_weight)
    input_pair, hidden_pair = swap(input_own), swap(hidden_own)
    (lead, starts, out_starts), frames, cell_start, gate_bias, first_weight, second_weight = (
        lax.optimization_barrier(
            ((lead, starts, out_starts), frames, cell_start, gate_bias, first_weight, second_weight)
        )
    )
    lead_parts = gathered(lead)
    input_both = (stage_call(input_own, input_pair),)
    hidden_both = (stage_call(hidden_own), hidden_pair[:, :, None])
    first_weight = stage_call(first_weight)
    second_weight = stage_call(second_weight)
    rest = ordered(frames_of(core, 1), swap(frames_of(1 - core, 1)), -1).reshape(steps - 1, count, width)
    cell_mine, cell_other = own_batch(cell_start, 0)
    cells = [cell_mine.reshape(count, share), cell_other.reshape(count, share)]
    bias_own = gate_bias.reshape(-1)
    bias = jnp.concatenate([bias_own, swap(bias_own)]).reshape(1, -1)

    lead_parts, cells, bias = lax.optimization_barrier((lead_parts, cells, bias))
    lead_edges = edges_of(lead_parts)
    rest_parts = forwarded(rest)
    next_edges = edges_of([part[:1] for part in rest_parts])
    later_edges = edges_of([part[1:] for part in rest_parts])

    for time_index in range(steps):
        if time_index == 0:
            parts, part_index, edges = lead_parts, 1, lead_edges
            image_parts, image_index, image_edges, edge_index = lead_parts, 0, lead_edges, 0
        else:
            parts, part_index = gathered(hidden), 0
            edges = edges_of(parts)
            image_parts, image_index = rest_parts, time_index - 1
            image_edges, edge_index = (next_edges, 0) if time_index == 1 else (later_edges, time_index - 2)
        late = time_index > 2
        total = conv_call(image_parts, image_index, image_edges if late else (), edge_index, input_both, bias, cols)
        sides = [] if late else [(image_edges, edge_index, input_both)]
        sides.append((edges, part_index, hidden_both))
        total = conv_call(parts, part_index, (), 0, hidden_both, total, cols)
        hidden, *cells = gate_call(sides, total, cells, cols, time_index == 0, time_index == steps - 1)

    image = jnp.pad(hidden.reshape(rows, cols, width), ((0, 0), (margin, margin), (0, 0)))

    def columns_for(k):
        piece = lax.dynamic_slice_in_dim(image, starts[k], tile, axis=1, allow_negative_indices=False)
        return piece.reshape(rows * tile, width)

    tiles = [columns_for(0)] + [
        lax.ppermute(columns_for(k), "hid", [(i, i ^ (2 * k)) for i in range(2 * groups)])
        for k in range(1, groups)
    ]
    rim = 2 * tile
    tile_edges = swapped_edges(
        jnp.stack([part[:rim] for part in tiles])[:, None],
        jnp.stack([part[rows * tile - rim :] for part in tiles])[:, None],
    )
    decoded = decoder_call(
        tiles, tile_edges, first_weight, first_bias, second_weight, second_bias, rows, tile, margin, inner
    )
    decoded = decoded.reshape(rows, tile, -1)
    mine, other = (
        lax.dynamic_slice_in_dim(decoded, start, inner // 2, axis=1, allow_negative_indices=False)
        for start in out_starts
    )
    other = swap(other)
    decoded = jnp.where(core == 0, jnp.stack([mine, other]), jnp.stack([other, mine]))

    cell_mine = cells[0].reshape(rows, cols, share)
    cell_other = swap(cells[1]).reshape(rows, cols, share)
    cell_final = jnp.where(core == 0, jnp.stack([cell_mine, cell_other]), jnp.stack([cell_other, cell_mine]))
    return decoded, cell_final


def solution(mesh):
    return jax.shard_map(
        program,
        mesh=mesh,
        in_specs=(
            P(None, None, "patch", None, "hid"),
            P(None, "patch", None, "hid"),
            P(None, "patch", None, "hid"),
            P(None, None, None, None, "hid"),
            P(None, None, None, None, "hid"),
            P(None, "hid"),
            P(),
            P(),
            P(),
            P(),
        ),
        out_specs=(P(None, "patch", "hid", None), P(None, "patch", None, "hid")),
        check_vma=False,
    )
```

```python
import functools

import jax
import jax.numpy as jnp
from jax import lax
from jax.experimental import pallas as pl
from jax.experimental.pallas import tpu as pltpu
from jax.sharding import PartitionSpec as P


FORGET_BIAS = 1.0
NT = (((1,), (1,)), ((), ()))
NN = (((1,), (0,)), ((), ()))


def place_columns(dst, row0, pieces, group, cols, masked):
    count, width = pieces[0].shape
    groups = len(pieces)
    place = lax.rem(lax.broadcasted_iota(jnp.int32, (count, width), 0), cols)

    def shifts(piece):
        wide = piece.astype(jnp.float32)
        low = pltpu.roll(wide, 1, 0)
        high = pltpu.roll(wide, count - 1, 0)
        if masked:
            low = jnp.where(place == 0, 0.0, low)
            high = jnp.where(place == cols - 1, 0.0, high)
        return (low.astype(dst.dtype), wide.astype(dst.dtype), high.astype(dst.dtype))

    shifted = [shifts(piece) for piece in pieces]
    rows = pl.ds(row0, count)
    if width % 128 == 0:
        for k in range(groups):
            lanes = pl.ds(pl.multiple_of(lax.bitwise_xor(group, k) * width, width), width)
            for q in range(3):
                dst[q, rows, lanes] = shifted[k][q]
    else:
        for j in range(groups):

            @pl.when(group == j)
            def _():
                for q in range(3):
                    dst[q, rows, :] = jnp.concatenate(
                        [shifted[j ^ i][q] for i in range(groups)], axis=1
                    )


def halo_pieces(a_ref, b_ref, index):
    patch = lax.axis_index("patch")
    even = lax.rem(patch, 2) == 0
    above = patch > 0
    below = patch < lax.axis_size("patch") - 1
    top, bottom = [], []
    for k in range(a_ref.shape[0]):
        a = a_ref[k, index].astype(jnp.float32)
        b = b_ref[k, index].astype(jnp.float32)
        top.append(jnp.where(above, jnp.where(even, b, a), 0.0))
        bottom.append(jnp.where(below, jnp.where(even, a, b), 0.0))
    return top, bottom


def stage_kernel(*refs):
    sources, target, semaphores = refs[:-2], refs[-2], refs[-1]
    copies = []
    for p in range(3):
        for q in range(3):
            for i, source in enumerate(sources):
                copy = pltpu.make_async_copy(source.at[p, q], target.at[p, q, i], semaphores.at[p, q, i])
                copy.start()
                copies.append(copy)
    for copy in copies:
        copy.wait()


def fetch_kernel(frames, hidden, cell, lead0, lead1, rest0, rest1, cell0, cell1, semaphores):
    core = lax.rem(lax.axis_index("hid"), 2)
    steps = frames.shape[0]
    copies = []
    for side, (lead, rest, kept) in enumerate(((lead0, rest0, cell0), (lead1, rest1, cell1))):
        index = core if side == 0 else 1 - core
        moves = [(frames.at[0, index], lead.at[0]), (hidden.at[index], lead.at[1])]
        moves += [(frames.at[t, index], rest.at[t - 1]) for t in range(1, steps)]
        moves += [(cell.at[index], kept)]
        copies += [
            pltpu.make_async_copy(source, target, semaphores.at[side, i]) for i, (source, target) in enumerate(moves)
        ]
    for copy in copies:
        copy.start()
    for copy in copies:
        copy.wait()


def tap(weight_refs, p, q):
    weights = [weight_ref[p, q] for weight_ref in weight_refs]
    weights = [weight.reshape(-1, weight.shape[-1]) for weight in weights]
    return weights[0] if len(weights) == 1 else jnp.concatenate(weights, axis=0)


def conv_kernel(groups, cols, index, edge_index, *refs):
    refs = list(refs)
    halo = edge_index is not None
    parts = [refs.pop(0) for _ in range(groups)]
    if halo:
        edge_a, edge_b = refs.pop(0), refs.pop(0)
    *weight_refs, out_ref, held = refs
    inits = [weight_refs.pop()]
    if inits[0].shape != out_ref.shape:
        inits.append(weight_refs.pop())
    count = out_ref.shape[1]
    group = lax.axis_index("hid") // 2

    place_columns(held, cols, [part[index] for part in parts], group, cols, True)
    if halo:
        top, bottom = halo_pieces(edge_a, edge_b, edge_index)
        place_columns(held, 0, top, group, cols, True)
        place_columns(held, cols + count, bottom, group, cols, True)
    else:
        zero = jnp.zeros((cols, held.shape[2]), held.dtype)
        for q in range(3):
            held[q, pl.ds(0, cols), :] = zero
            held[q, pl.ds(cols + count, cols), :] = zero
    if len(inits) == 1:
        total = inits[0][...]
    else:
        turned = jnp.concatenate([inits[1][...], inits[0][...]]).T
        total = jnp.concatenate(
            [jnp.broadcast_to(turned[:, i : i + 1], (turned.shape[0], count)) for i in range(turned.shape[1])]
        )
    for p in range(3):
        for q in range(3):
            window = held[q, p * cols : p * cols + count, :]
            total = total + lax.dot_general(
                tap(weight_refs, p, q), window, NT, preferred_element_type=jnp.float32
            )
    out_ref[...] = total


def add_edges(sides, summed, held, cols):
    group = lax.axis_index("hid") // 2
    count = summed.shape[1]
    side = 2 * cols
    zero = jnp.zeros((cols, held.shape[2]), held.dtype)
    for q in range(3):
        held[q, pl.ds(cols, cols), :] = zero
        held[q, pl.ds(2 * cols, cols), :] = zero
    for edge_a, edge_b, weight_refs, index in sides:
        top, bottom = halo_pieces(edge_a, edge_b, index)
        place_columns(held, 0, top, group, cols, True)
        place_columns(held, 3 * cols, bottom, group, cols, True)
        for p, row0, lane0 in ((0, 0, 0), (2, side, count - side)):
            total = summed[:, lane0 : lane0 + side]
            for q in range(3):
                window = held[q, row0 : row0 + side, :]
                total = total + lax.dot_general(
                    tap(weight_refs, p, q), window, NT, preferred_element_type=jnp.float32
                )
            summed[:, lane0 : lane0 + side] = total


def side_kernel(cols, index, edge_a, edge_b, *refs):
    *weight_refs, total_ref, out_ref, held = refs
    out_ref[...] = total_ref[...]
    add_edges([(edge_a, edge_b, weight_refs, index)], out_ref, held, cols)


def gate_kernel(cols, indices, turn_in, turn_out, *refs):
    refs = list(refs)
    sides = []
    for index, pieces in indices:
        sides.append((refs.pop(0), refs.pop(0), [refs.pop(0) for _ in range(pieces)], index))
    total_ref = refs.pop(0)
    cells = [refs.pop(0), refs.pop(0)]
    hidden_ref = refs.pop(0)
    cells_out = [refs.pop(0), refs.pop(0)]
    held, turned, summed = refs
    core = lax.rem(lax.axis_index("hid"), 2)
    channels = total_ref.shape[0] // 8

    summed[...] = total_ref[...]
    add_edges(sides, summed, held, cols)
    for half in range(2):
        base = half * 4 * channels
        z0, z1, z2, z3 = (summed[base + i * channels : base + (i + 1) * channels, :] for i in range(4))
        cell = cells[half][...].T if turn_in else cells[half][...]
        cell = jax.nn.sigmoid(z1 + FORGET_BIAS) * cell + jax.nn.sigmoid(z0) * jnp.tanh(z2)
        cells_out[half][...] = cell.T if turn_out else cell
        rows = pl.ds(pl.multiple_of(lax.bitwise_xor(core, half) * channels, channels), channels)
        turned[rows, :] = jax.nn.sigmoid(z3) * jnp.tanh(cell)
    hidden_ref[0] = turned[...].T.astype(hidden_ref.dtype)


def decoder_kernel(groups, rows, width, margin, inner, *refs):
    parts = refs[:groups]
    edge_a, edge_b, first_ref, bias1_ref, second_ref, bias2_ref, out_ref, held, middle = refs[groups:]
    group = lax.axis_index("hid") // 2
    patch = lax.axis_index("patch")
    image_rows = rows * lax.axis_size("patch")
    image_cols = inner * groups

    def conv(source, weight_ref, bias_ref, count):
        total = jnp.broadcast_to(bias_ref[...], (count * width, bias_ref.shape[1]))
        for p in range(3):
            for q in range(3):
                window = source[q, p * width : (p + count) * width, :]
                total = total + lax.dot_general(
                    window, tap([weight_ref], p, q), NN, preferred_element_type=jnp.float32
                )
        return total

    top, bottom = halo_pieces(edge_a, edge_b, 0)
    place_columns(held, 0, top, group, width, False)
    place_columns(held, 2 * width, [part[...] for part in parts], group, width, False)
    place_columns(held, (2 + rows) * width, bottom, group, width, False)
    value = conv(held, first_ref, bias1_ref, rows + 2)
    place = lax.broadcasted_iota(jnp.int32, value.shape, 0)
    row = patch * rows + place // width - 1
    col = group * inner - margin + lax.rem(place, width)
    inside = (row >= 0) & (row < image_rows) & (col >= 0) & (col < image_cols)
    value = jnp.where(inside, value * jax.nn.sigmoid(value), 0.0)
    value = value.astype(middle.dtype).astype(jnp.float32)
    middle[0] = pltpu.roll(value, 1, 0).astype(middle.dtype)
    middle[1] = value.astype(middle.dtype)
    middle[2] = pltpu.roll(value, value.shape[0] - 1, 0).astype(middle.dtype)
    out_ref[...] = conv(middle, second_ref, bias2_ref, rows).astype(out_ref.dtype)


WHOLE = pl.BlockSpec(memory_space=pltpu.VMEM)
VMEM_LIMIT = 10 * 1024 * 1024


def params():
    return pltpu.CompilerParams(vmem_limit_bytes=VMEM_LIMIT)


def cost(flops, size):
    return pl.CostEstimate(flops=flops, bytes_accessed=size, transcendentals=0)


def stage_call(*sources):
    shape = sources[0].shape[:2] + (len(sources),) + sources[0].shape[2:]
    size = 2 * sources[0].size * len(sources)
    return pl.pallas_call(
        stage_kernel,
        in_specs=[pl.BlockSpec(memory_space=pltpu.HBM)] * len(sources),
        out_specs=WHOLE,
        out_shape=pltpu.VMEM(shape, sources[0].dtype),
        scratch_shapes=[pltpu.SemaphoreType.DMA((3, 3, len(sources)))],
        compiler_params=params(),
        cost_estimate=cost(100 * size, size),
    )(*(pltpu.with_memory_space_constraint(source, pltpu.HBM) for source in sources))


def fetch_call(frames, hidden, cell):
    steps, _, *block = frames.shape
    pair = [pltpu.VMEM((2, *block), frames.dtype)] * 2
    pair += [pltpu.VMEM((steps - 1, *block), frames.dtype)] * 2
    pair += [pltpu.VMEM(tuple(block), cell.dtype)] * 2
    return pl.pallas_call(
        fetch_kernel,
        in_specs=[pl.BlockSpec(memory_space=pltpu.HBM)] * 3,
        out_specs=[WHOLE] * 6,
        out_shape=pair,
        scratch_shapes=[pltpu.SemaphoreType.DMA((2, steps + 2))],
        compiler_params=params(),
        cost_estimate=cost(1000, 4 * frames.size),
    )(*(pltpu.with_memory_space_constraint(source, pltpu.HBM) for source in (frames, hidden, cell)))


def side_call(edges, index, weights, total, cols):
    operands = [*edges, *weights, total]
    return pl.pallas_call(
        functools.partial(side_kernel, cols, index),
        in_specs=[WHOLE] * len(operands),
        out_specs=WHOLE,
        out_shape=jax.ShapeDtypeStruct(total.shape, total.dtype),
        scratch_shapes=[pltpu.VMEM((3, 4 * cols, weights[0].shape[-1]), jnp.bfloat16)],
        compiler_params=params(),
        cost_estimate=cost(3 * total.size * weights[0].shape[-1], 4 * total.size),
    )(*operands)


def conv_call(parts, index, edges, edge_index, weights, inits, cols):
    groups = len(parts)
    count = parts[0].shape[1]
    channels = weights[0].shape[-1]
    outs = 2 * weights[0].shape[3]
    operands = [*parts, *edges, *weights, *inits]
    return pl.pallas_call(
        functools.partial(conv_kernel, groups, cols, index, edge_index if edges else None),
        in_specs=[WHOLE] * len(operands),
        out_specs=WHOLE,
        out_shape=jax.ShapeDtypeStruct((outs, count), jnp.float32),
        scratch_shapes=[pltpu.VMEM((3, count + 2 * cols, channels), jnp.bfloat16)],
        compiler_params=params(),
        cost_estimate=cost(2 * outs * count * 9 * channels, 18 * outs * channels),
    )(*operands)


def gate_call(sides, total, cells, cols, turn_in, turn_out):
    outs, count = total.shape
    channels = sides[0][2][0].shape[-1]
    share = outs // 8
    width = 2 * share
    cell_shape = (count, share) if turn_out else (share, count)
    operands = []
    for edges, _, weights in sides:
        operands += [*edges, *weights]
    operands += [total, *cells]
    return pl.pallas_call(
        functools.partial(gate_kernel, cols, [(index, len(weights)) for _, index, weights in sides], turn_in, turn_out),
        in_specs=[WHOLE] * len(operands),
        out_specs=[WHOLE] * 3,
        out_shape=[jax.ShapeDtypeStruct((1, count, width), jnp.bfloat16)]
        + [jax.ShapeDtypeStruct(cell_shape, jnp.float32)] * 2,
        scratch_shapes=[
            pltpu.VMEM((3, 4 * cols, channels), jnp.bfloat16),
            pltpu.VMEM((width, count), jnp.float32),
            pltpu.VMEM((outs, count), jnp.float32),
        ],
        compiler_params=params(),
        cost_estimate=cost(2 * outs * count * 6 * channels, 12 * outs * channels),
    )(*operands)


def decoder_call(parts, edges, first, first_bias, second, second_bias, rows, width, margin, inner):
    groups = len(parts)
    channels = first.shape[3]
    outs = second.shape[4]
    operands = [*parts, *edges, first, first_bias.reshape(1, -1), second, second_bias.reshape(1, -1)]
    return pl.pallas_call(
        functools.partial(decoder_kernel, groups, rows, width, margin, inner),
        in_specs=[WHOLE] * len(operands),
        out_specs=WHOLE,
        out_shape=jax.ShapeDtypeStruct((rows * width, outs), jnp.bfloat16),
        scratch_shapes=[
            pltpu.VMEM((3, (rows + 4) * width, channels), jnp.bfloat16),
            pltpu.VMEM((3, (rows + 2) * width, first.shape[4]), jnp.bfloat16),
        ],
        compiler_params=params(),
        cost_estimate=cost(18 * channels * outs * (2 * rows + 2) * width, 36 * channels * outs),
    )(*operands)


def program(
    frames,
    hidden_start,
    cell_start,
    input_weight,
    hidden_weight,
    gate_bias,
    first_weight,
    first_bias,
    second_weight,
    second_bias,
):
    steps, batch, rows, cols, share = frames.shape
    groups = lax.axis_size("hid") // 2
    patches = lax.axis_size("patch")
    assert batch == 2 and groups & (groups - 1) == 0 and patches % 2 == 0
    hid = lax.axis_index("hid")
    core = lax.rem(hid, 2)
    group = hid // 2
    even = lax.rem(lax.axis_index("patch"), 2) == 0
    count = rows * cols
    width = 2 * share

    pairs = [(i, i ^ 1) for i in range(2 * groups)]
    inner_pairs = [(i, i ^ 1) for i in range(patches)]
    outer_pairs = [(i, (i - 1) % patches if i % 2 == 0 else (i + 1) % patches) for i in range(patches)]

    def swap(value):
        return lax.ppermute(value, "hid", pairs)

    def gathered(value):
        return [value] + [
            lax.ppermute(value, "hid", [(i, i ^ (2 * k)) for i in range(2 * groups)]) for k in range(1, groups)
        ]

    def across(value, k):
        return lax.ppermute(value, "hid", [(i, i ^ (2 * k)) for i in range(2 * groups)])

    def forwarded(value):
        parts = [value]
        parts += [across(value, k) for k in range(1, groups) if k == 1 or k % 2 == 0]
        near = dict(zip([0, 1] + [k for k in range(2, groups, 2)], parts))
        for k in range(3, groups, 2):
            near[k] = across(near[k - 1], 1)
        return [near[k] for k in range(groups)]

    def swapped_edges(top, bottom):
        first = lax.ppermute(jnp.where(even, bottom, top), "patch", inner_pairs)
        second = lax.ppermute(jnp.where(even, top, bottom), "patch", outer_pairs)
        return first, second

    def edges_of(parts):
        top = jnp.stack([part[:, :cols] for part in parts])
        bottom = jnp.stack([part[:, count - cols :] for part in parts])
        return swapped_edges(top, bottom)

    def gate_major(weight):
        turned = jnp.transpose(weight, (0, 1, 3, 4, 2))
        return turned.reshape(turned.shape[:2] + (-1,) + turned.shape[-1:])

    def ordered(mine, other, axis):
        return jnp.where(core == 0, jnp.concatenate([mine, other], axis), jnp.concatenate([other, mine], axis))

    lead_mine, lead_other, rest_mine, rest_other, cell_mine, cell_other = fetch_call(frames, hidden_start, cell_start)
    lead = ordered(lead_mine, swap(lead_other), -1).reshape(2, count, width)
    inner = cols // groups
    tile = -(-(inner + 4) // 16) * 16
    margin = (tile - inner) // 2
    starts = [lax.bitwise_xor(group, k) * inner for k in range(groups)]
    out_starts = [margin + core * (inner // 2), margin + (1 - core) * (inner // 2)]
    input_own, hidden_own = gate_major(input_weight), gate_major(hidden_weight)
    input_pair, hidden_pair = swap(input_own), swap(hidden_own)
    (lead, starts, out_starts), rest_other, cell_other, gate_bias, first_weight, second_weight = (
        lax.optimization_barrier(
            ((lead, starts, out_starts), rest_other, cell_other, gate_bias, first_weight, second_weight)
        )
    )
    lead_parts = gathered(lead)
    input_both = (stage_call(input_own, input_pair),)
    hidden_both = (stage_call(hidden_own), hidden_pair[:, :, None])
    first_weight = stage_call(first_weight)
    second_weight = stage_call(second_weight)
    rest = ordered(rest_mine, swap(rest_other), -1).reshape(steps - 1, count, width)
    rest = lax.optimization_barrier(rest)
    cells = [cell.reshape(count, share) for cell in (cell_mine, swap(cell_other))]
    bias = [gate_bias, swap(gate_bias)]

    lead_parts, cells, bias = lax.optimization_barrier((lead_parts, cells, bias))
    lead_edges = edges_of(lead_parts)
    rest_parts = forwarded(rest)
    next_edges = edges_of([part[:1] for part in rest_parts])
    later_edges = edges_of([part[1:] for part in rest_parts])

    for time_index in range(steps):
        if time_index == 0:
            parts, part_index, edges = lead_parts, 1, lead_edges
            image_parts, image_index, image_edges, edge_index = lead_parts, 0, lead_edges, 0
        else:
            parts, part_index = gathered(hidden), 0
            edges = edges_of(parts)
            image_parts, image_index = rest_parts, time_index - 1
            image_edges, edge_index = (next_edges, 0) if time_index == 1 else (later_edges, time_index - 2)
        late = time_index > 2
        total = conv_call(image_parts, image_index, image_edges if late else (), edge_index, input_both, bias, cols)
        sides = [(image_edges, edge_index, input_both)] if time_index == 0 else []
        sides.append((edges, part_index, hidden_both))
        total = conv_call(parts, part_index, (), 0, hidden_both, [total], cols)
        if 0 < time_index and not late:
            total = side_call(image_edges, edge_index, input_both, total, cols)
        hidden, *cells = gate_call(sides, total, cells, cols, time_index == 0, time_index == steps - 1)

    image = jnp.pad(hidden.reshape(rows, cols, width), ((0, 0), (margin, margin), (0, 0)))

    def columns_for(k):
        piece = lax.dynamic_slice_in_dim(image, starts[k], tile, axis=1, allow_negative_indices=False)
        return piece.reshape(rows * tile, width)

    tiles = [columns_for(0)] + [
        lax.ppermute(columns_for(k), "hid", [(i, i ^ (2 * k)) for i in range(2 * groups)])
        for k in range(1, groups)
    ]
    rim = 2 * tile
    tile_edges = swapped_edges(
        jnp.stack([part[:rim] for part in tiles])[:, None],
        jnp.stack([part[rows * tile - rim :] for part in tiles])[:, None],
    )
    decoded = decoder_call(
        tiles, tile_edges, first_weight, first_bias, second_weight, second_bias, rows, tile, margin, inner
    )
    decoded = decoded.reshape(rows, tile, -1)
    mine, other = (
        lax.dynamic_slice_in_dim(decoded, start, inner // 2, axis=1, allow_negative_indices=False)
        for start in out_starts
    )
    other = swap(other)
    decoded = jnp.where(core == 0, jnp.stack([mine, other]), jnp.stack([other, mine]))

    cell_mine = cells[0].reshape(rows, cols, share)
    cell_other = swap(cells[1]).reshape(rows, cols, share)
    cell_final = jnp.where(core == 0, jnp.stack([cell_mine, cell_other]), jnp.stack([cell_other, cell_mine]))
    return decoded, cell_final


def solution(mesh):
    return jax.shard_map(
        program,
        mesh=mesh,
        in_specs=(
            P(None, None, "patch", None, "hid"),
            P(None, "patch", None, "hid"),
            P(None, "patch", None, "hid"),
            P(None, None, None, None, "hid"),
            P(None, None, None, None, "hid"),
            P(None, "hid"),
            P(),
            P(),
            P(),
            P(),
        ),
        out_specs=(P(None, "patch", "hid", None), P(None, "patch", None, "hid")),
        check_vma=False,
    )
```

```python
import functools

import jax
import jax.numpy as jnp
from jax import lax
from jax.experimental import pallas as pl
from jax.experimental.pallas import tpu as pltpu
from jax.sharding import PartitionSpec as P


FORGET_BIAS = 1.0
NT = (((1,), (1,)), ((), ()))
NN = (((1,), (0,)), ((), ()))


def place_columns(dst, row0, pieces, group, cols, masked):
    count, width = pieces[0].shape
    groups = len(pieces)
    place = lax.rem(lax.broadcasted_iota(jnp.int32, (count, width), 0), cols)

    def shifts(piece):
        wide = piece.astype(jnp.float32)
        low = pltpu.roll(wide, 1, 0)
        high = pltpu.roll(wide, count - 1, 0)
        if masked:
            low = jnp.where(place == 0, 0.0, low)
            high = jnp.where(place == cols - 1, 0.0, high)
        return (low.astype(dst.dtype), wide.astype(dst.dtype), high.astype(dst.dtype))

    shifted = [shifts(piece) for piece in pieces]
    rows = pl.ds(row0, count)
    if width % 128 == 0:
        for k in range(groups):
            lanes = pl.ds(pl.multiple_of(lax.bitwise_xor(group, k) * width, width), width)
            for q in range(3):
                dst[q, rows, lanes] = shifted[k][q]
    else:
        for j in range(groups):

            @pl.when(group == j)
            def _():
                for q in range(3):
                    dst[q, rows, :] = jnp.concatenate(
                        [shifted[j ^ i][q] for i in range(groups)], axis=1
                    )


def halo_pieces(a_ref, b_ref, index):
    patch = lax.axis_index("patch")
    even = lax.rem(patch, 2) == 0
    above = patch > 0
    below = patch < lax.axis_size("patch") - 1
    top, bottom = [], []
    for k in range(a_ref.shape[0]):
        a = a_ref[k, index].astype(jnp.float32)
        b = b_ref[k, index].astype(jnp.float32)
        top.append(jnp.where(above, jnp.where(even, b, a), 0.0))
        bottom.append(jnp.where(below, jnp.where(even, a, b), 0.0))
    return top, bottom


def stage_kernel(*refs):
    sources, target, semaphores = refs[:-2], refs[-2], refs[-1]
    copies = []
    for p in range(3):
        for q in range(3):
            for i, source in enumerate(sources):
                copy = pltpu.make_async_copy(source.at[p, q], target.at[p, q, i], semaphores.at[p, q, i])
                copy.start()
                copies.append(copy)
    for copy in copies:
        copy.wait()


def fetch_kernel(frames, hidden, cell, lead0, lead1, rest0, rest1, cell0, cell1, semaphores):
    core = lax.rem(lax.axis_index("hid"), 2)
    steps = frames.shape[0]
    copies = []
    for side, (lead, rest, kept) in enumerate(((lead0, rest0, cell0), (lead1, rest1, cell1))):
        index = core if side == 0 else 1 - core
        moves = [(frames.at[0, index], lead.at[0]), (hidden.at[index], lead.at[1])]
        moves += [(frames.at[t, index], rest.at[t - 1]) for t in range(1, steps)]
        moves += [(cell.at[index], kept)]
        copies += [
            pltpu.make_async_copy(source, target, semaphores.at[side, i]) for i, (source, target) in enumerate(moves)
        ]
    for copy in copies:
        copy.start()
    for copy in copies:
        copy.wait()


def tap(weight_refs, p, q):
    weights = [weight_ref[p, q] for weight_ref in weight_refs]
    weights = [weight.reshape(-1, weight.shape[-1]) for weight in weights]
    return weights[0] if len(weights) == 1 else jnp.concatenate(weights, axis=0)


def conv_kernel(groups, cols, index, edge_index, *refs):
    refs = list(refs)
    halo = edge_index is not None
    parts = [refs.pop(0) for _ in range(groups)]
    if halo:
        edge_a, edge_b = refs.pop(0), refs.pop(0)
    *weight_refs, out_ref, held = refs
    inits = [weight_refs.pop()]
    if inits[0].shape != out_ref.shape:
        inits.append(weight_refs.pop())
    count = out_ref.shape[1]
    group = lax.axis_index("hid") // 2

    place_columns(held, cols, [part[index] for part in parts], group, cols, True)
    if halo:
        top, bottom = halo_pieces(edge_a, edge_b, edge_index)
        place_columns(held, 0, top, group, cols, True)
        place_columns(held, cols + count, bottom, group, cols, True)
    else:
        zero = jnp.zeros((cols, held.shape[2]), held.dtype)
        for q in range(3):
            held[q, pl.ds(0, cols), :] = zero
            held[q, pl.ds(cols + count, cols), :] = zero
    if len(inits) == 1:
        total = inits[0][...]
    else:
        turned = jnp.concatenate([inits[1][...], inits[0][...]]).T
        total = jnp.concatenate(
            [jnp.broadcast_to(turned[:, i : i + 1], (turned.shape[0], count)) for i in range(turned.shape[1])]
        )
    for p in range(3):
        for q in range(3):
            window = held[q, p * cols : p * cols + count, :]
            total = total + lax.dot_general(
                tap(weight_refs, p, q), window, NT, preferred_element_type=jnp.float32
            )
    out_ref[...] = total


def add_edges(sides, summed, held, cols):
    group = lax.axis_index("hid") // 2
    count = summed.shape[1]
    side = 2 * cols
    zero = jnp.zeros((cols, held.shape[2]), held.dtype)
    for q in range(3):
        held[q, pl.ds(cols, cols), :] = zero
        held[q, pl.ds(2 * cols, cols), :] = zero
    for edge_a, edge_b, weight_refs, index in sides:
        top, bottom = halo_pieces(edge_a, edge_b, index)
        place_columns(held, 0, top, group, cols, True)
        place_columns(held, 3 * cols, bottom, group, cols, True)
        for p, row0, lane0 in ((0, 0, 0), (2, side, count - side)):
            total = summed[:, lane0 : lane0 + side]
            for q in range(3):
                window = held[q, row0 : row0 + side, :]
                total = total + lax.dot_general(
                    tap(weight_refs, p, q), window, NT, preferred_element_type=jnp.float32
                )
            summed[:, lane0 : lane0 + side] = total


def side_kernel(cols, index, edge_a, edge_b, *refs):
    *weight_refs, total_ref, out_ref, held = refs
    out_ref[...] = total_ref[...]
    add_edges([(edge_a, edge_b, weight_refs, index)], out_ref, held, cols)


def gate_kernel(cols, indices, turn_in, turn_out, *refs):
    refs = list(refs)
    sides = []
    for index, pieces in indices:
        sides.append((refs.pop(0), refs.pop(0), [refs.pop(0) for _ in range(pieces)], index))
    total_ref = refs.pop(0)
    cells = [refs.pop(0), refs.pop(0)]
    hidden_ref = refs.pop(0)
    cells_out = [refs.pop(0), refs.pop(0)]
    held, turned, summed = refs
    core = lax.rem(lax.axis_index("hid"), 2)
    channels = total_ref.shape[0] // 8

    summed[...] = total_ref[...]
    add_edges(sides, summed, held, cols)
    for half in range(2):
        base = half * 4 * channels
        z0, z1, z2, z3 = (summed[base + i * channels : base + (i + 1) * channels, :] for i in range(4))
        cell = cells[half][...].T if turn_in else cells[half][...]
        cell = jax.nn.sigmoid(z1 + FORGET_BIAS) * cell + jax.nn.sigmoid(z0) * jnp.tanh(z2)
        cells_out[half][...] = cell.T if turn_out else cell
        rows = pl.ds(pl.multiple_of(lax.bitwise_xor(core, half) * channels, channels), channels)
        turned[rows, :] = jax.nn.sigmoid(z3) * jnp.tanh(cell)
    hidden_ref[0] = turned[...].T.astype(hidden_ref.dtype)


def decoder_kernel(groups, rows, width, margin, inner, *refs):
    parts = refs[:groups]
    edge_a, edge_b, first_ref, bias1_ref, second_ref, bias2_ref, out_ref, held, middle = refs[groups:]
    group = lax.axis_index("hid") // 2
    patch = lax.axis_index("patch")
    image_rows = rows * lax.axis_size("patch")
    image_cols = inner * groups

    def conv(source, weight_ref, bias_ref, count):
        total = jnp.broadcast_to(bias_ref[...], (count * width, bias_ref.shape[1]))
        for p in range(3):
            for q in range(3):
                window = source[q, p * width : (p + count) * width, :]
                total = total + lax.dot_general(
                    window, tap([weight_ref], p, q), NN, preferred_element_type=jnp.float32
                )
        return total

    top, bottom = halo_pieces(edge_a, edge_b, 0)
    place_columns(held, 0, top, group, width, False)
    place_columns(held, 2 * width, [part[...] for part in parts], group, width, False)
    place_columns(held, (2 + rows) * width, bottom, group, width, False)
    value = conv(held, first_ref, bias1_ref, rows + 2)
    place = lax.broadcasted_iota(jnp.int32, value.shape, 0)
    row = patch * rows + place // width - 1
    col = group * inner - margin + lax.rem(place, width)
    inside = (row >= 0) & (row < image_rows) & (col >= 0) & (col < image_cols)
    value = jnp.where(inside, value * jax.nn.sigmoid(value), 0.0)
    value = value.astype(middle.dtype).astype(jnp.float32)
    middle[0] = pltpu.roll(value, 1, 0).astype(middle.dtype)
    middle[1] = value.astype(middle.dtype)
    middle[2] = pltpu.roll(value, value.shape[0] - 1, 0).astype(middle.dtype)
    out_ref[...] = conv(middle, second_ref, bias2_ref, rows).astype(out_ref.dtype)


WHOLE = pl.BlockSpec(memory_space=pltpu.VMEM)
VMEM_LIMIT = 10 * 1024 * 1024


def params():
    return pltpu.CompilerParams(vmem_limit_bytes=VMEM_LIMIT)


def cost(flops, size):
    return pl.CostEstimate(flops=flops, bytes_accessed=size, transcendentals=0)


def stage_call(*sources):
    shape = sources[0].shape[:2] + (len(sources),) + sources[0].shape[2:]
    size = 2 * sources[0].size * len(sources)
    return pl.pallas_call(
        stage_kernel,
        in_specs=[pl.BlockSpec(memory_space=pltpu.HBM)] * len(sources),
        out_specs=WHOLE,
        out_shape=pltpu.VMEM(shape, sources[0].dtype),
        scratch_shapes=[pltpu.SemaphoreType.DMA((3, 3, len(sources)))],
        compiler_params=params(),
        cost_estimate=cost(100 * size, size),
    )(*(pltpu.with_memory_space_constraint(source, pltpu.HBM) for source in sources))


def fetch_call(frames, hidden, cell):
    steps, _, *block = frames.shape
    pair = [pltpu.VMEM((2, *block), frames.dtype)] * 2
    pair += [pltpu.VMEM((steps - 1, *block), frames.dtype)] * 2
    pair += [pltpu.VMEM(tuple(block), cell.dtype)] * 2
    return pl.pallas_call(
        fetch_kernel,
        in_specs=[pl.BlockSpec(memory_space=pltpu.HBM)] * 3,
        out_specs=[WHOLE] * 6,
        out_shape=pair,
        scratch_shapes=[pltpu.SemaphoreType.DMA((2, steps + 2))],
        compiler_params=params(),
        cost_estimate=cost(1000, 4 * frames.size),
    )(*(pltpu.with_memory_space_constraint(source, pltpu.HBM) for source in (frames, hidden, cell)))


def side_call(edges, index, weights, total, cols):
    operands = [*edges, *weights, total]
    return pl.pallas_call(
        functools.partial(side_kernel, cols, index),
        in_specs=[WHOLE] * len(operands),
        out_specs=WHOLE,
        out_shape=jax.ShapeDtypeStruct(total.shape, total.dtype),
        scratch_shapes=[pltpu.VMEM((3, 4 * cols, weights[0].shape[-1]), jnp.bfloat16)],
        compiler_params=params(),
        cost_estimate=cost(3 * total.size * weights[0].shape[-1], 4 * total.size),
    )(*operands)


def conv_call(parts, index, edges, edge_index, weights, inits, cols):
    groups = len(parts)
    count = parts[0].shape[1]
    channels = weights[0].shape[-1]
    outs = 2 * weights[0].shape[3]
    operands = [*parts, *edges, *weights, *inits]
    return pl.pallas_call(
        functools.partial(conv_kernel, groups, cols, index, edge_index if edges else None),
        in_specs=[WHOLE] * len(operands),
        out_specs=WHOLE,
        out_shape=jax.ShapeDtypeStruct((outs, count), jnp.float32),
        scratch_shapes=[pltpu.VMEM((3, count + 2 * cols, channels), jnp.bfloat16)],
        compiler_params=params(),
        cost_estimate=cost(2 * outs * count * 9 * channels, 18 * outs * channels),
    )(*operands)


def gate_call(sides, total, cells, cols, turn_in, turn_out):
    outs, count = total.shape
    channels = sides[0][2][0].shape[-1]
    share = outs // 8
    width = 2 * share
    cell_shape = (count, share) if turn_out else (share, count)
    operands = []
    for edges, _, weights in sides:
        operands += [*edges, *weights]
    operands += [total, *cells]
    return pl.pallas_call(
        functools.partial(gate_kernel, cols, [(index, len(weights)) for _, index, weights in sides], turn_in, turn_out),
        in_specs=[WHOLE] * len(operands),
        out_specs=[WHOLE] * 3,
        out_shape=[jax.ShapeDtypeStruct((1, count, width), jnp.bfloat16)]
        + [jax.ShapeDtypeStruct(cell_shape, jnp.float32)] * 2,
        scratch_shapes=[
            pltpu.VMEM((3, 4 * cols, channels), jnp.bfloat16),
            pltpu.VMEM((width, count), jnp.float32),
            pltpu.VMEM((outs, count), jnp.float32),
        ],
        compiler_params=params(),
        cost_estimate=cost(2 * outs * count * 6 * channels, 12 * outs * channels),
    )(*operands)


def decoder_call(parts, edges, first, first_bias, second, second_bias, rows, width, margin, inner):
    groups = len(parts)
    channels = first.shape[3]
    outs = second.shape[4]
    operands = [*parts, *edges, first, first_bias.reshape(1, -1), second, second_bias.reshape(1, -1)]
    return pl.pallas_call(
        functools.partial(decoder_kernel, groups, rows, width, margin, inner),
        in_specs=[WHOLE] * len(operands),
        out_specs=WHOLE,
        out_shape=jax.ShapeDtypeStruct((rows * width, outs), jnp.bfloat16),
        scratch_shapes=[
            pltpu.VMEM((3, (rows + 4) * width, channels), jnp.bfloat16),
            pltpu.VMEM((3, (rows + 2) * width, first.shape[4]), jnp.bfloat16),
        ],
        compiler_params=params(),
        cost_estimate=cost(18 * channels * outs * (2 * rows + 2) * width, 36 * channels * outs),
    )(*operands)


def program(
    frames,
    hidden_start,
    cell_start,
    input_weight,
    hidden_weight,
    gate_bias,
    first_weight,
    first_bias,
    second_weight,
    second_bias,
):
    steps, batch, rows, cols, share = frames.shape
    groups = lax.axis_size("hid") // 2
    patches = lax.axis_size("patch")
    assert batch == 2 and groups & (groups - 1) == 0 and patches % 2 == 0
    hid = lax.axis_index("hid")
    core = lax.rem(hid, 2)
    group = hid // 2
    even = lax.rem(lax.axis_index("patch"), 2) == 0
    count = rows * cols
    width = 2 * share

    pairs = [(i, i ^ 1) for i in range(2 * groups)]
    inner_pairs = [(i, i ^ 1) for i in range(patches)]
    outer_pairs = [(i, (i - 1) % patches if i % 2 == 0 else (i + 1) % patches) for i in range(patches)]

    def swap(value):
        return lax.ppermute(value, "hid", pairs)

    def gathered(value):
        return [value] + [
            lax.ppermute(value, "hid", [(i, i ^ (2 * k)) for i in range(2 * groups)]) for k in range(1, groups)
        ]

    def across(value, k):
        return lax.ppermute(value, "hid", [(i, i ^ (2 * k)) for i in range(2 * groups)])

    def forwarded(value):
        parts = [value]
        parts += [across(value, k) for k in range(1, groups) if k == 1 or k % 2 == 0]
        near = dict(zip([0, 1] + [k for k in range(2, groups, 2)], parts))
        for k in range(3, groups, 2):
            near[k] = across(near[k - 1], 1)
        return [near[k] for k in range(groups)]

    def swapped_edges(top, bottom):
        first = lax.ppermute(jnp.where(even, bottom, top), "patch", inner_pairs)
        second = lax.ppermute(jnp.where(even, top, bottom), "patch", outer_pairs)
        return first, second

    def edges_of(parts):
        top = jnp.stack([part[:, :cols] for part in parts])
        bottom = jnp.stack([part[:, count - cols :] for part in parts])
        return swapped_edges(top, bottom)

    def gate_major(weight):
        turned = jnp.transpose(weight, (0, 1, 3, 4, 2))
        return turned.reshape(turned.shape[:2] + (-1,) + turned.shape[-1:])

    def ordered(mine, other, axis):
        return jnp.where(core == 0, jnp.concatenate([mine, other], axis), jnp.concatenate([other, mine], axis))

    lead_mine, lead_other, rest_mine, rest_other, cell_mine, cell_other = fetch_call(frames, hidden_start, cell_start)
    lead = ordered(lead_mine, swap(lead_other), -1).reshape(2, count, width)
    inner = cols // groups
    tile = -(-(inner + 4) // 16) * 16
    margin = (tile - inner) // 2
    starts = [lax.bitwise_xor(group, k) * inner for k in range(groups)]
    out_starts = [margin + core * (inner // 2), margin + (1 - core) * (inner // 2)]
    input_own, hidden_own = gate_major(input_weight), gate_major(hidden_weight)
    input_pair, hidden_pair = swap(input_own), swap(hidden_own)
    (lead, starts, out_starts), rest_other, cell_other, gate_bias, first_weight, second_weight = (
        lax.optimization_barrier(
            ((lead, starts, out_starts), rest_other, cell_other, gate_bias, first_weight, second_weight)
        )
    )
    lead_parts = gathered(lead)
    input_both = (stage_call(input_own, input_pair),)
    hidden_both = (stage_call(hidden_own), hidden_pair[:, :, None])
    first_weight = stage_call(first_weight)
    second_weight = stage_call(second_weight)
    rest = ordered(rest_mine, swap(rest_other), -1).reshape(steps - 1, count, width)
    rest = lax.optimization_barrier(rest)
    cells = [cell.reshape(count, share) for cell in (cell_mine, swap(cell_other))]
    bias = [gate_bias, swap(gate_bias)]

    lead_parts, cells, bias = lax.optimization_barrier((lead_parts, cells, bias))
    lead_edges = edges_of(lead_parts)
    rest_parts = forwarded(rest)
    next_edges = edges_of([part[:1] for part in rest_parts])
    later_edges = edges_of([part[1:] for part in rest_parts])

    for time_index in range(steps):
        if time_index == 0:
            parts, part_index, edges = lead_parts, 1, lead_edges
            image_parts, image_index, image_edges, edge_index = lead_parts, 0, lead_edges, 0
        else:
            parts, part_index = gathered(hidden), 0
            edges = edges_of(parts)
            image_parts, image_index = rest_parts, time_index - 1
            image_edges, edge_index = (next_edges, 0) if time_index == 1 else (later_edges, time_index - 2)
        late = time_index > 2
        total = conv_call(image_parts, image_index, image_edges if late else (), edge_index, input_both, bias, cols)
        sides = [(image_edges, edge_index, input_both)] if time_index == 0 else []
        sides.append((edges, part_index, hidden_both))
        total = conv_call(parts, part_index, (), 0, hidden_both, [total], cols)
        if 0 < time_index and not late:
            total = side_call(image_edges, edge_index, input_both, total, cols)
        hidden, *cells = gate_call(sides, total, cells, cols, time_index == 0, time_index == steps - 1)

    image = jnp.pad(hidden.reshape(rows, cols, width), ((0, 0), (margin, margin), (0, 0)))

    def columns_for(k):
        piece = lax.dynamic_slice_in_dim(image, starts[k], tile, axis=1, allow_negative_indices=False)
        return piece.reshape(rows * tile, width)

    tiles = [columns_for(0)]
    for k in range(1, groups):
        tiles.append(lax.ppermute(columns_for(k), "hid", [(i, i ^ (2 * k)) for i in range(2 * groups)]))
    rim = 2 * tile
    tile_edges = swapped_edges(
        jnp.stack([part[:rim] for part in tiles])[:, None],
        jnp.stack([part[rows * tile - rim :] for part in tiles])[:, None],
    )
    decoded = decoder_call(
        tiles, tile_edges, first_weight, first_bias, second_weight, second_bias, rows, tile, margin, inner
    )
    decoded = decoded.reshape(rows, tile, -1)
    mine, other = (
        lax.dynamic_slice_in_dim(decoded, start, inner // 2, axis=1, allow_negative_indices=False)
        for start in out_starts
    )
    other = swap(other)
    decoded = jnp.where(core == 0, jnp.stack([mine, other]), jnp.stack([other, mine]))

    cell_mine = cells[0].reshape(rows, cols, share)
    cell_other = swap(cells[1]).reshape(rows, cols, share)
    cell_final = jnp.where(core == 0, jnp.stack([cell_mine, cell_other]), jnp.stack([cell_other, cell_mine]))
    return decoded, cell_final


def solution(mesh):
    return jax.shard_map(
        program,
        mesh=mesh,
        in_specs=(
            P(None, None, "patch", None, "hid"),
            P(None, "patch", None, "hid"),
            P(None, "patch", None, "hid"),
            P(None, None, None, None, "hid"),
            P(None, None, None, None, "hid"),
            P(None, "hid"),
            P(),
            P(),
            P(),
            P(),
        ),
        out_specs=(P(None, "patch", "hid", None), P(None, "patch", None, "hid")),
        check_vma=False,
    )
```
